256 devices in a mesh: dp: 8 (over z_lo, core), expert: 32 (over y, x, z_hi).
Axes of the slice: x: 4, y: 4, z: 8 (z_hi: 2, z_lo: 4; z = z_hi * 4 + z_lo), core: 2. Of those that a mesh axis runs over, the one named last changes fastest.
Arguments:
- tokens: bfloat16 [32768, 3584], P(('dp', 'expert')), may hold values from -6 to 6
- cotangent: bfloat16 [32768, 3584], P(('dp', 'expert')), may hold values from -6 to 6
- gates: float32 [32768, 1], P(('dp', 'expert')), may hold values from 0.1 to 1
- routes: int32 [32768, 1], P(('dp', 'expert')), may hold values from 0 to 31; in each aligned block of 128 rows (0 to 127, 128 to 255, ...) at most 5 rows name the same one
- w_up: bfloat16 [32, 3584, 1024], P('expert', None, 'dp'), may hold values from -0.09375 to 0.09375
- w_down: bfloat16 [32, 1024, 3584], P('expert', 'dp'), may hold values from -0.1875 to 0.1875
- m_up: bfloat16 [32, 3584, 1024], P('expert', None, 'dp'), may hold values from -3 to 3
- v_up: bfloat16 [32, 3584, 1024], P('expert', None, 'dp'), may hold values from 0.099609375 to 1
- m_down: bfloat16 [32, 1024, 3584], P('expert', 'dp'), may hold values from -3 to 3
- v_down: bfloat16 [32, 1024, 3584], P('expert', 'dp'), may hold values from 0.099609375 to 1
- leaving: int32 [1], replicated, may hold values from 0 to 31
- tile_owner: int32 [32], replicated, may hold values from 0 to 31, each once
Outputs:
- update_up: bfloat16 [32, 3584, 1024], P('expert', None, 'dp')
- update_down: bfloat16 [32, 1024, 3584], P('expert', 'dp')
- adopted_up: bfloat16 [32, 112, 1024], P('expert', None, 'dp')
- adopted_down: bfloat16 [32, 112, 1024], P('expert', None, 'dp')
The draws below stay inside these ranges and needn't reach their ends.
Inputs may be any that keep to these rules, and one draw needn't show every extreme that they name: `routes`: each row names one expert; within the 128 rows of one device no expert is named more than 5 times, a bound that some block reaches in some devices. `tile_owner`: A permutation of the 32 device indices of the expert axis.
All inputs are finite; a program needn't handle non-finite values.
Results may differ from the reference program's by a relative error of at most 0.0041.
Values may be sent and summed in bfloat16 or wider, within the bound.
No kernel may reach another device: no remote copies, remote signals or barrier semaphores. Data moves between devices by JAX's collectives and lax.ppermute only.
A program may use at most 128 MiB of HBM per device.

```python
import math
import jax
import jax.numpy as jnp
import numpy as np
from jax import lax

D = 3584
FF = 1024
TOK_DEV = 128
TOPK = 1
EXPERTS = 32
TOKENS = 32768
CAP = 5
DEVICES = 256


def level_of(key, shape, shards, smallest, largest):
    factor_of, own = 1.0, jax.random.fold_in(key, 6)
    for position, shards_of in shards:
        heights = jnp.exp(jax.random.uniform(jax.random.fold_in(own, position), (shards_of,), jnp.float32, smallest / len(shards), largest / len(shards)))
        factor_of = factor_of * jnp.repeat(heights, shape[position] // shards_of).reshape([-1 if axis == position else 1 for axis in range(len(shape))])
    return factor_of


def deal_out(stream_key, own, number, rows, count, top, reach, skew):
    order = jax.random.permutation(stream_key, count)
    packed, ordinary = portions_of(count, rows * top, reach, skew, True), portions_of(count, rows * top, reach, skew, False)
    places = jnp.arange(count)

    def named(sizes, rotation):
        used = int((sizes > 0).sum())
        fixed = max(1, used // 4)
        shifted = fixed + (places - fixed + rotation * (used - fixed)) % max(1, count - fixed)
        return jnp.zeros((count,), jnp.int32).at[order[jnp.where(places < fixed, places, shifted)]].set(jnp.asarray(sizes, jnp.int32))

    sizes = jnp.where(number % 4 == 0, named(packed, number // 4), named(ordinary, number - number // 4 - 1))
    mixed = jax.random.permutation(jax.random.fold_in(own, 3), count)
    giver, receiver = mixed[0:count // 2 * 2:2], mixed[1:count // 2 * 2:2]
    room = jnp.minimum(sizes[giver] - 1, reach - sizes[receiver]) // 2
    room = jnp.where((giver == order[0]) | (receiver == order[0]) | (sizes[receiver] == 0), 0, jnp.maximum(room, 0))
    shifted = jax.random.randint(jax.random.fold_in(own, 4), (count // 2,), 0, 1 << 20) % (room + 1)
    sizes = sizes.at[giver].add(-shifted).at[receiver].add(shifted)
    labels = jnp.searchsorted(jnp.cumsum(sizes), jnp.arange(rows * top), side="right").astype(jnp.int32)
    listing = labels.reshape(top, rows).T
    listing = listing[jax.random.permutation(jax.random.fold_in(own, 1), rows)]
    rotation = jax.random.randint(jax.random.fold_in(own, 2), (rows, 1), 0, top)
    return jnp.take_along_axis(listing, (jnp.arange(top)[None, :] + rotation) % top, axis=1)


def portions_of(number_of, total, bound, lean, full):
    weights = [(1 << 20) // math.isqrt(grade ** lean) + 1 for grade in range(1, number_of + 1)]
    largest = bound if full else min(bound, max(-(-total // number_of), total * weights[0] // sum(weights)))
    least = 1 if total - largest >= number_of - 1 else 0
    holding, rest = [largest] + [least] * (number_of - 1), total - largest - least * (number_of - 1)
    while rest > 0:
        candidates = [i for i in range(1, number_of) if holding[i] < largest] or [i for i in range(1, number_of) if holding[i] < bound]
        whole, remaining = sum([weights[i] for i in candidates]), rest
        for i in candidates:
            addition = min(bound - holding[i], max(1, remaining * weights[i] // whole), rest)
            holding[i] = holding[i] + addition
            rest = rest - addition
    return np.array(holding)


def centred(key, dims, spread, limit, split=(), kind=jnp.bfloat16):
    drawn = jax.random.normal(key, dims, jnp.float32) * spread
    if len(split) > 0:
        drawn = level_of(key, dims, split, -0.22, 0.18) * drawn
    return jnp.clip(drawn, min=-limit, max=limit).astype(kind)


def setup_inputs(seed: int = 0) -> dict:
    streams_of = jax.random.split(jax.random.key(seed), 13)
    tokens = centred(streams_of[0], (TOKENS, D), 1.0, 6.0, ((0, 256),))
    cotangent = centred(streams_of[1], (TOKENS, D), 1.0, 6.0, ((0, 256),))
    gates = jnp.clip(jnp.exp(math.log(1.0) - 2.3025851 * jax.random.uniform(streams_of[2], (TOKENS, TOPK), jnp.float32) ** level_of(streams_of[2], (TOKENS, TOPK), ((0, 256),), -0.2, 0.2)), 0.1, 1.0)
    routes_keys = jax.random.split(jax.random.fold_in(streams_of[3], 1), TOKENS // TOK_DEV)
    routes_turns = jax.random.permutation(jax.random.fold_in(streams_of[3], 3), TOKENS // TOK_DEV)
    routes = jax.vmap(lambda own, number: deal_out(jax.random.fold_in(streams_of[3], 2), own, number, TOK_DEV, EXPERTS, TOPK, CAP, 1))(routes_keys, routes_turns).reshape((TOKENS, TOPK))
    w_up = centred(streams_of[4], (EXPERTS, D, FF), D ** -0.5, 0.09375, ((0, 32), (2, 8)))
    w_down = centred(streams_of[5], (EXPERTS, FF, D), FF ** -0.5, 0.1875, ((0, 32), (1, 8)))
    m_up = centred(streams_of[6], (EXPERTS, D, FF), 0.5, 3.0, ((0, 32), (2, 8)))
    v_up = jnp.clip(jnp.exp(math.log(1.0) - 2.306499 * jax.random.uniform(streams_of[7], (EXPERTS, D, FF), jnp.float32) ** level_of(streams_of[7], (EXPERTS, D, FF), ((0, 32), (2, 8)), -0.2, 0.2)), 0.099609375, 1.0).astype(jnp.bfloat16)
    m_down = centred(streams_of[8], (EXPERTS, FF, D), 0.5, 3.0, ((0, 32), (1, 8)))
    v_down = jnp.clip(jnp.exp(math.log(1.0) - 2.306499 * jax.random.uniform(streams_of[9], (EXPERTS, FF, D), jnp.float32) ** level_of(streams_of[9], (EXPERTS, FF, D), ((0, 32), (1, 8)), -0.2, 0.2)), 0.099609375, 1.0).astype(jnp.bfloat16)
    leaving = jax.random.randint(streams_of[10], (1,), 0, EXPERTS).astype(jnp.int32)
    tile_owner = jax.random.permutation(streams_of[11], EXPERTS).astype(jnp.int32)
    return {"tokens": tokens, "cotangent": cotangent, "gates": gates, "routes": routes, "w_up": w_up, "w_down": w_down, "m_up": m_up, "v_up": v_up, "m_down": m_down, "v_down": v_down, "leaving": leaving, "tile_owner": tile_owner}


BETA_ONE = 0.9
BETA_TWO = 0.95
EPSILON = 1e-08

def expert_terms(rows_x, rows_c, up_tile, down_tile):
    preact = jnp.dot(rows_x, up_tile, preferred_element_type=jnp.float32)
    squash = jax.nn.sigmoid(preact)
    hidden = (preact * squash).astype(jnp.bfloat16)
    slope_val = squash * (1.0 + preact * (1.0 - squash))
    back_grad = lax.dot_general(rows_c, down_tile, (((1,), (1,)), ((), ())), preferred_element_type=jnp.float32)
    pre_grad = (back_grad * slope_val).astype(jnp.bfloat16)
    grad_up = lax.dot_general(rows_x, pre_grad, (((0,), (0,)), ((), ())), preferred_element_type=jnp.float32)
    grad_cols = lax.dot_general(rows_c, hidden, (((0,), (0,)), ((), ())), preferred_element_type=jnp.float32)
    return (grad_up, grad_cols)

def adam_step(gradient, moment_one, moment_two):
    new_one = BETA_ONE * moment_one.astype(jnp.float32) + (1.0 - BETA_ONE) * gradient
    new_two = BETA_TWO * moment_two.astype(jnp.float32) + (1.0 - BETA_TWO) * gradient * gradient
    return (new_one / (jnp.sqrt(new_two) + EPSILON)).astype(jnp.bfloat16)

def reference(tokens, cotangent, gates, routes, w_up, w_down, m_up, v_up, m_down, v_down, leaving, tile_owner):
    experts = w_up.shape[0]
    hidden_units = w_up.shape[2]
    tok_count, model_width = tokens.shape
    top_count = routes.shape[1]
    pair_count = tok_count * top_count
    expert_of = routes.reshape(pair_count)
    pair_x = jnp.repeat(tokens, top_count, axis=0)
    pair_c = (gates.reshape(pair_count)[:, None] * jnp.repeat(cotangent, top_count, axis=0).astype(jnp.float32)).astype(jnp.bfloat16)
    most_rows = DEVICES * CAP

    def one_expert(expert_id):
        sort_key = jnp.where(expert_of == expert_id, 0, 1).astype(jnp.int32)
        row_order = jnp.argsort(sort_key, stable=True)[:most_rows]
        is_valid = (expert_of[row_order] == expert_id)[:, None]
        rows_x = jnp.where(is_valid, pair_x[row_order], jnp.zeros((), jnp.bfloat16))
        rows_c = jnp.where(is_valid, pair_c[row_order], jnp.zeros((), jnp.bfloat16))
        up_tile = lax.dynamic_index_in_dim(w_up, expert_id, 0, keepdims=False)
        down_tile = lax.dynamic_index_in_dim(w_down, expert_id, 0, keepdims=False)
        grad_up, grad_cols = expert_terms(rows_x, rows_c, up_tile, down_tile)
        step_up = adam_step(grad_up, lax.dynamic_index_in_dim(m_up, expert_id, 0, keepdims=False), lax.dynamic_index_in_dim(v_up, expert_id, 0, keepdims=False))
        step_down = adam_step(grad_cols.T, lax.dynamic_index_in_dim(m_down, expert_id, 0, keepdims=False), lax.dynamic_index_in_dim(v_down, expert_id, 0, keepdims=False))
        return (step_up, step_down)
    expert_ids = jnp.arange(experts, dtype=jnp.int32)
    steps_up, steps_down = lax.map(one_expert, expert_ids)
    leaver = leaving[0]
    keep_own = (expert_ids != leaver)[:, None, None]
    update_up = jnp.where(keep_own, steps_up, jnp.zeros((), jnp.bfloat16))
    update_down = jnp.where(keep_own, steps_down, jnp.zeros((), jnp.bfloat16))
    leaver_up = lax.dynamic_index_in_dim(steps_up, leaver, 0, keepdims=False)
    leaver_down = lax.dynamic_index_in_dim(steps_down, leaver, 0, keepdims=False)
    tile_rows = model_width // experts
    adopt = lax.optimization_barrier(jnp.sum(jnp.where(tile_owner[None, :] == expert_ids[:, None], expert_ids[None, :], 0), axis=1)).astype(jnp.int32)
    adopted_up = leaver_up.reshape(experts, tile_rows, hidden_units)[adopt]
    adopted_down = leaver_down.T.reshape(experts, tile_rows, hidden_units)[adopt]
    return (update_up, update_down, adopted_up, adopted_down)
```

```python
import jax
import jax.numpy as jnp
from jax import lax
from jax.experimental import pallas as pl
from jax.experimental.pallas import tpu as pltpu
from jax.sharding import Mesh
from jax.sharding import PartitionSpec as P

BETA_ONE = 0.9
BETA_TWO = 0.95
EPSILON = 1e-08

ALL = ("zl", "co", "y", "x", "zh")
SLOT_GROUPS = ((0, 2), (2, 3))
PIECES = 4
VMEM = pl.BlockSpec(memory_space=pltpu.VMEM)
SMEM = pl.BlockSpec(memory_space=pltpu.SMEM)
LIMIT = 60 * 1024 * 1024


def device_id(z, core, y, x):
    return (((z % 4) * 2 + core) * 4 + y) * 8 + x * 2 + z // 4


def every():
    for z in range(8):
        for core in range(2):
            for y in range(4):
                for x in range(4):
                    yield z, core, y, x


def stream_pairs(places):
    pairs = []
    for z, core, y, x in every():
        place = z % 4 if core == 0 else 3 - z % 4
        if place in places:
            there = (z + (1 if core == 0 else -1)) % 8
            pairs.append((device_id(z, core, y, x), device_id(there, core, y, x)))
    return pairs


def swap_pairs():
    return [(device_id(z, c, y, x), device_id(z, 1 - c, y, x)) for z, c, y, x in every()]


def across_pairs():
    return [(device_id(z, c, y, x), device_id((z + 4) % 8, c, y, x)) for z, c, y, x in every()]


def over(value, divisor):
    if divisor & (divisor - 1) == 0:
        return value >> (divisor.bit_length() - 1)
    return (value * (-(-(1 << 18) // divisor))) >> 18


def prepare(base, tokens, cotangent, gates_row, routes_row, outs_slots):
    tok_count, width = tokens.shape
    piece = width // PIECES
    parts = 2 * PIECES

    def body(base_ref, x_ref, c_ref, g_ref, r_ref, *rest):
        outs, (held,) = rest[:-1], rest[-1:]
        routes = jnp.broadcast_to(r_ref[...], (tok_count, tok_count))
        routes_down = routes.T
        gate_down = jnp.broadcast_to(g_ref[...], (tok_count, tok_count)).T
        at_row = lax.broadcasted_iota(jnp.int32, (tok_count, tok_count), 0)
        at_col = lax.broadcasted_iota(jnp.int32, (tok_count, tok_count), 1)
        before = jnp.where((routes_down == routes) & (at_row < at_col), 1, 0)
        rank = jnp.sum(before, axis=0, keepdims=True)
        code = r_ref[...] * 8 + rank
        for q in range(PIECES):
            held[q * tok_count : (q + 1) * tok_count, :] = x_ref[:, q * piece : (q + 1) * piece]
            for j in range(piece // 128):
                cols = c_ref[:, q * piece + j * 128 : q * piece + (j + 1) * 128]
                held[
                    (PIECES + q) * tok_count : (PIECES + q + 1) * tok_count,
                    j * 128 : (j + 1) * 128,
                ] = (gate_down * cols.astype(jnp.float32)).astype(jnp.bfloat16)
        for out, (first, slots) in zip(outs, outs_slots):
            rows = 32 * parts * slots
            row = lax.broadcasted_iota(jnp.int32, (rows, tok_count), 0)
            group = over(row, slots)
            slot = row - group * slots
            part = group & (parts - 1)
            dest = group >> 3
            expert = ((dest & 15) << 1) | (base_ref[0] ^ (dest >> 4))
            hit = (expert * 8 + (slot + first)) == code
            picker = jnp.concatenate(
                [
                    jnp.where(hit & (part == q), 1.0, 0.0).astype(jnp.bfloat16)
                    for q in range(parts)
                ],
                axis=1,
            )
            out[...] = jnp.dot(
                picker, held[...], preferred_element_type=jnp.float32
            ).astype(jnp.bfloat16)

    return pl.pallas_call(
        body,
        out_shape=[
            jax.ShapeDtypeStruct((32 * parts * slots, piece), jnp.bfloat16)
            for _, slots in outs_slots
        ],
        in_specs=[SMEM, VMEM, VMEM, VMEM, VMEM],
        out_specs=[VMEM] * len(outs_slots),
        scratch_shapes=[pltpu.VMEM((parts * tok_count, piece), jnp.bfloat16)],
        compiler_params=pltpu.CompilerParams(vmem_limit_bytes=LIMIT),
        name="prepare",
    )(base, tokens, cotangent, gates_row, routes_row)


def sorter(slots):
    rows = 16 * 8 * slots
    row = lax.broadcasted_iota(jnp.int32, (rows, rows), 0)
    col = lax.broadcasted_iota(jnp.int32, (rows, rows), 1)
    part = over(row, 16 * slots)
    rest = row - part * (16 * slots)
    sender = over(rest, slots)
    slot = rest - sender * slots
    return jnp.where(col == sender * (8 * slots) + part * slots + slot, 1.0, 0.0).astype(
        jnp.bfloat16
    )


def absorb(place, blocks, w_up, w_down, sums):
    arrays = []
    for _, _, first, second in blocks:
        arrays.append(first)
        if second is not None:
            arrays.append(second)
    width, hidden_units = w_up.shape
    piece = width // PIECES
    total = sum(32 * slots for slots, _, _, _ in blocks)
    have = sums is not None

    def body(place_ref, *refs):
        ins, refs = list(refs[: len(arrays)]), refs[len(arrays) :]
        up_ref, down_ref = refs[:2]
        refs = refs[2:]
        if have:
            old_up, old_down = refs[:2]
            refs = refs[2:]
        out_up, out_down, held = refs
        at = place_ref[0]
        sorters = {}
        offset = 0
        for slots, test, _, second in blocks:
            if slots not in sorters:
                sorters[slots] = sorter(slots)
            first_ref = ins.pop(0)
            second_ref = ins.pop(0) if second is not None else None
            rows, count = 16 * 8 * slots, 16 * slots
            for half in range(2):
                span = slice(half * rows, (half + 1) * rows)
                block = first_ref[span, :]
                if second_ref is not None:
                    block = jnp.where(test(at), block, second_ref[span, :])
                ordered = jnp.dot(sorters[slots], block, preferred_element_type=jnp.float32)
                for q in range(2 * PIECES):
                    part = ordered[q * count : (q + 1) * count, :]
                    if second_ref is None and test is not None and q >= PIECES:
                        part = jnp.where(test(at), part, 0.0)
                    held[q, offset : offset + count, :] = part.astype(jnp.bfloat16)
                offset += count
        preact = sum(
            jnp.dot(
                held[q],
                up_ref[q * piece : (q + 1) * piece, :],
                preferred_element_type=jnp.float32,
            )
            for q in range(PIECES)
        )
        back_grad = sum(
            lax.dot_general(
                held[PIECES + q],
                down_ref[:, q * piece : (q + 1) * piece],
                (((1,), (1,)), ((), ())),
                preferred_element_type=jnp.float32,
            )
            for q in range(PIECES)
        )
        squash = jax.nn.sigmoid(preact)
        hidden = (preact * squash).astype(jnp.bfloat16)
        slope = squash * (1.0 + preact * (1.0 - squash))
        pre_grad = (back_grad * slope).astype(jnp.bfloat16)
        for q in range(PIECES):
            span = slice(q * piece, (q + 1) * piece)
            for left, right, old, out in (
                (pre_grad, held[q], old_up if have else None, out_up),
                (hidden, held[PIECES + q], old_down if have else None, out_down),
            ):
                part = lax.dot_general(
                    left, right, (((0,), (0,)), ((), ())), preferred_element_type=jnp.float32
                )
                out[:, span] = part + old[:, span] if have else part

    shape = jax.ShapeDtypeStruct((hidden_units, width), jnp.float32)
    args = [place, *arrays, w_up, w_down] + (list(sums) if have else [])
    flops = 8 * total * width * hidden_units
    return pl.pallas_call(
        body,
        out_shape=[shape, shape],
        in_specs=[SMEM] + [VMEM] * (len(args) - 1),
        out_specs=[VMEM, VMEM],
        scratch_shapes=[pltpu.VMEM((2 * PIECES, total, piece), jnp.bfloat16)],
        input_output_aliases={len(args) - 2: 0, len(args) - 1: 1} if have else {},
        compiler_params=pltpu.CompilerParams(vmem_limit_bytes=LIMIT),
        cost_estimate=pl.CostEstimate(
            flops=flops, transcendentals=0, bytes_accessed=16 * total * width
        ),
        name="absorb",
    )(*args)


def adam_step(gradient, moment_one, moment_two):
    new_one = BETA_ONE * moment_one.astype(jnp.float32) + (1.0 - BETA_ONE) * gradient
    new_two = BETA_TWO * moment_two.astype(jnp.float32) + (1.0 - BETA_TWO) * gradient * gradient
    return new_one / (jnp.sqrt(new_two) + EPSILON)


def finish(my_index, leaving, tile_owner, sums, m_up, v_up, m_down, v_down):
    width, hidden_units = m_up.shape
    tiles = tile_owner.shape[0]
    tile_rows = width // tiles

    def body(me, leave, owner, gu, gd, mu, vu, md, vd, out_up, out_down, out_tiles, both):
        keep = me[0] != leave[0]
        for j in range(width // 128):
            span = slice(j * 128, (j + 1) * 128)
            step_up = adam_step(gu[:, span].T, mu[span, :], vu[span, :])
            both[span, :hidden_units] = step_up.astype(jnp.bfloat16)
            out_up[span, :] = jnp.where(keep, step_up, 0.0).astype(jnp.bfloat16)
            step_down = adam_step(gd[:, span], md[:, span], vd[:, span])
            both[span, hidden_units:] = step_down.T.astype(jnp.bfloat16)
            out_down[:, span] = jnp.where(keep, step_down, 0.0).astype(jnp.bfloat16)
        for t in range(tiles):
            out_tiles[owner[t]] = both[t * tile_rows : (t + 1) * tile_rows, :]

    return pl.pallas_call(
        body,
        out_shape=[
            jax.ShapeDtypeStruct((width, hidden_units), jnp.bfloat16),
            jax.ShapeDtypeStruct((hidden_units, width), jnp.bfloat16),
            jax.ShapeDtypeStruct((tiles, tile_rows, 2 * hidden_units), jnp.bfloat16),
        ],
        in_specs=[SMEM, SMEM, SMEM] + [VMEM] * 6,
        out_specs=[VMEM] * 3,
        scratch_shapes=[pltpu.VMEM((width, 2 * hidden_units), jnp.bfloat16)],
        compiler_params=pltpu.CompilerParams(vmem_limit_bytes=LIMIT),
        name="finish",
    )(my_index, leaving, tile_owner, *sums, m_up, v_up, m_down, v_down)


def on_device(
    tokens, cotangent, gates, routes, w_up, w_down, m_up, v_up, m_down, v_down, leaving, tile_owner
):
    tok_count, width = tokens.shape
    piece = width // PIECES
    core = lax.axis_index("co")
    low = lax.axis_index("zl")
    half = lax.axis_index("zh")
    column = lax.axis_index(("y", "x"))
    place = jnp.where(core == 0, low, 3 - low)
    base = jnp.where(low <= 1, half, 1 - half)
    place_ref = place.reshape(1)

    outgoing = prepare(
        base.reshape(1),
        tokens,
        cotangent,
        gates.reshape(1, tok_count),
        routes.reshape(1, tok_count),
        SLOT_GROUPS,
    )

    def step(value, places):
        return lax.ppermute(value, ALL, stream_pairs(places))

    def swap(value):
        return lax.ppermute(value, ALL, swap_pairs())

    chunks = []
    for (_, slots), sent in zip(SLOT_GROUPS, outgoing):
        rows = sent.shape[0]
        first = lax.all_to_all(
            sent.reshape(32, rows // 32, piece), ("co", "y", "x"), 0, 0, tiled=True
        ).reshape(rows, piece)
        chunks.append({"slots": slots, 0: first})
    for ch in chunks:
        ch["s0"] = swap(ch[0])
        ch[1] = step(ch[0], (0, 1, 2, 3))
    for ch in chunks:
        ch[2] = step(jnp.where(place == 2, ch["s0"], ch[1]), (0, 1, 2, 3))
        ch["s1"] = swap(ch[1])
    for ch in chunks:
        ch[3] = step(jnp.where(place == 2, ch[1], ch[2]), (0, 1, 2))
        ch["s2"] = swap(ch[2])
    for ch in chunks:
        ch[4] = step(jnp.where(place == 2, ch[2], ch[3]), (1, 2))
        ch["s3"] = swap(ch[3])
    for ch in chunks:
        ch[5] = step(ch[3], (2,))
        ch["s4"] = swap(ch[4])
    for ch in chunks:
        ch[6] = step(ch[4], (2,))
        ch["s5"] = swap(ch[5])
    for ch in chunks:
        ch["s6"] = swap(ch[6])

    groups = [
        [(lambda at: at <= 1, 0, "s0"), (lambda at: at < 3, 1, None), (lambda at: at > 0, "s1", None)],
        [(None, 2, None), (None, "s2", None)],
        [(None, 3, None), (None, "s3", None), (lambda at: at >= 2, 4, "s4")],
        [(lambda at: at == 3, 5, "s5")],
        [(lambda at: at == 3, 6, "s6")],
    ]
    sums = None
    for group in groups:
        blocks = [
            (ch["slots"], test, ch[a], None if b is None else ch[b])
            for ch in chunks
            for test, a, b in group
        ]
        sums = absorb(place_ref, blocks, w_up[0], w_down[0], sums)

    my_index = (column * 2 + half).reshape(1)
    update_up, update_down, tiles = finish(
        my_index, leaving, tile_owner, sums, m_up[0], v_up[0], m_down[0], v_down[0]
    )
    units = w_up.shape[2]
    tile_rows = tiles.shape[1]
    incoming = lax.all_to_all(
        tiles.reshape(16, 2, tile_rows, 2 * units), ("y", "x"), 0, 0, tiled=True
    )
    leaver = leaving[0]
    pair = lax.dynamic_index_in_dim(incoming, leaver // 2, 0, keepdims=False)
    own = lax.dynamic_index_in_dim(pair, half, 0, keepdims=False)
    other = lax.dynamic_index_in_dim(pair, 1 - half, 0, keepdims=False)
    mine = jnp.where(half == leaver % 2, own, lax.ppermute(other, ALL, across_pairs()))
    return (update_up[None], update_down[None], mine[None, :, :units], mine[None, :, units:])


def solution(mesh):
    wide = Mesh(mesh.devices.reshape(4, 2, 4, 4, 2), ALL)
    dp = ("zl", "co")
    expert = ("y", "x", "zh")
    row = P(dp + expert, None)
    up = P(expert, None, dp)
    down = P(expert, dp, None)
    return jax.shard_map(
        on_device,
        mesh=wide,
        in_specs=(row, row, row, row, up, down, up, up, down, down, P(), P()),
        out_specs=(up, down, up, up),
        check_vma=False,
    )
```

```python
import jax
import jax.numpy as jnp
from jax import lax
from jax.experimental import pallas as pl
from jax.experimental.pallas import tpu as pltpu
from jax.sharding import Mesh
from jax.sharding import PartitionSpec as P


BETA_ONE = 0.9
BETA_TWO = 0.95
EPSILON = 1e-08

ALL = ("zl", "co", "y", "x", "zh")
SLOT_GROUPS = ((0, 2), (2, 3))
TAGS = ("a", "b")
SUMS = ("ao1p2q3r", "a45 bo1p", "b2q", "b3r4 a6", "b5")
LAST = "b6"
PIECES = 4
VMEM = pl.BlockSpec(memory_space=pltpu.VMEM)
SMEM = pl.BlockSpec(memory_space=pltpu.SMEM)
LIMIT = 60 * 1024 * 1024


def device_id(z, core, y, x):
    return (((z % 4) * 2 + core) * 4 + y) * 8 + x * 2 + z // 4


def every():
    for z in range(8):
        for core in range(2):
            for y in range(4):
                for x in range(4):
                    yield z, core, y, x


def stream_pairs(places):
    pairs = []
    for z, core, y, x in every():
        place = z % 4 if core == 0 else 3 - z % 4
        if place in places:
            there = (z + (1 if core == 0 else -1)) % 8
            pairs.append((device_id(z, core, y, x), device_id(there, core, y, x)))
    return pairs


def swap_pairs():
    return [(device_id(z, c, y, x), device_id(z, 1 - c, y, x)) for z, c, y, x in every()]


def across_pairs():
    return [(device_id(z, c, y, x), device_id((z + 4) % 8, c, y, x)) for z, c, y, x in every()]


def over(value, divisor):
    if divisor & (divisor - 1) == 0:
        return value >> (divisor.bit_length() - 1)
    return (value * (-(-(1 << 18) // divisor))) >> 18


def prepare(base, tokens, cotangent, gates_row, routes_row, outs_slots):
    tok_count, width = tokens.shape
    piece = width // PIECES
    parts = 2 * PIECES

    def body(base_ref, x_ref, c_ref, g_ref, r_ref, *rest):
        outs, (held,) = rest[:-1], rest[-1:]
        routes = jnp.broadcast_to(r_ref[...], (tok_count, tok_count))
        routes_down = routes.T
        gate_down = jnp.broadcast_to(g_ref[...], (tok_count, tok_count)).T
        at_row = lax.broadcasted_iota(jnp.int32, (tok_count, tok_count), 0)
        at_col = lax.broadcasted_iota(jnp.int32, (tok_count, tok_count), 1)
        before = jnp.where((routes_down == routes) & (at_row < at_col), 1, 0)
        rank = jnp.sum(before, axis=0, keepdims=True)
        code = r_ref[...] * 8 + rank
        for q in range(PIECES):
            held[q * tok_count : (q + 1) * tok_count, :] = x_ref[:, q * piece : (q + 1) * piece]
            for j in range(piece // 128):
                cols = c_ref[:, q * piece + j * 128 : q * piece + (j + 1) * 128]
                held[
                    (PIECES + q) * tok_count : (PIECES + q + 1) * tok_count,
                    j * 128 : (j + 1) * 128,
                ] = (gate_down * cols.astype(jnp.float32)).astype(jnp.bfloat16)
        for out, (first, slots) in zip(outs, outs_slots):
            rows = 32 * parts * slots
            row = lax.broadcasted_iota(jnp.int32, (rows, tok_count), 0)
            group = over(row, slots)
            slot = row - group * slots
            part = group & (parts - 1)
            dest = group >> 3
            expert = ((dest & 15) << 1) | (base_ref[0] ^ (dest >> 4))
            hit = (expert * 8 + (slot + first)) == code
            picker = jnp.concatenate(
                [
                    jnp.where(hit & (part == q), 1.0, 0.0).astype(jnp.bfloat16)
                    for q in range(parts)
                ],
                axis=1,
            )
            out[...] = jnp.dot(
                picker, held[...], preferred_element_type=jnp.float32
            ).astype(jnp.bfloat16)

    return pl.pallas_call(
        body,
        out_shape=[
            jax.ShapeDtypeStruct((32 * parts * slots, piece), jnp.bfloat16)
            for _, slots in outs_slots
        ],
        in_specs=[SMEM, VMEM, VMEM, VMEM, VMEM],
        out_specs=[VMEM] * len(outs_slots),
        scratch_shapes=[pltpu.VMEM((parts * tok_count, piece), jnp.bfloat16)],
        compiler_params=pltpu.CompilerParams(vmem_limit_bytes=LIMIT),
        name="prepare",
    )(base, tokens, cotangent, gates_row, routes_row)


def sorter(slots):
    rows = 16 * 8 * slots
    row = lax.broadcasted_iota(jnp.int32, (rows, rows), 0)
    col = lax.broadcasted_iota(jnp.int32, (rows, rows), 1)
    part = over(row, 16 * slots)
    rest = row - part * (16 * slots)
    sender = over(rest, slots)
    slot = rest - sender * slots
    return jnp.where(col == sender * (8 * slots) + part * slots + slot, 1.0, 0.0).astype(
        jnp.bfloat16
    )


def arrange(received, slots):
    _, piece = received.shape
    count = 16 * slots

    def body(in_ref, out_ref):
        order = sorter(slots)
        for half in range(2):
            block = in_ref[half * 8 * count : (half + 1) * 8 * count, :]
            ordered = jnp.dot(order, block, preferred_element_type=jnp.float32)
            ordered = ordered.astype(jnp.bfloat16)
            for q in range(2 * PIECES):
                out_ref[q, half * count : (half + 1) * count, :] = ordered[
                    q * count : (q + 1) * count, :
                ]

    return pl.pallas_call(
        body,
        out_shape=jax.ShapeDtypeStruct((2 * PIECES, 2 * count, piece), jnp.bfloat16),
        in_specs=[VMEM],
        out_specs=VMEM,
        compiler_params=pltpu.CompilerParams(vmem_limit_bytes=LIMIT),
        name="arrange",
    )(received)


def flatten(blocks):
    arrays = []
    for _, first, second in blocks:
        arrays.append(first)
        if second is not None:
            arrays.append(second)
    return arrays


def gather_rows(at, blocks, refs, held_x, held_c):
    refs = list(refs)
    piece = refs[0].shape[2]
    offset = 0
    for test, _, second in blocks:
        first_ref = refs.pop(0)
        second_ref = refs.pop(0) if second is not None else None
        count = first_ref.shape[1]
        for q in range(2 * PIECES):
            part = first_ref[q]
            if second_ref is not None:
                part = jnp.where(test(at), part, second_ref[q])
            elif test is not None and q >= PIECES:
                part = jnp.where(test(at), part, jnp.zeros_like(part))
            held = held_x if q < PIECES else held_c
            left = (q % PIECES) * piece
            held[offset : offset + count, left : left + piece] = part
        offset += count


def row_terms(up_ref, down_ref, held_x, held_c, held_pre, held_hid, tile):
    def rows_of(i, carry):
        span = pl.ds(pl.multiple_of(i * tile, tile), tile)
        preact = jnp.dot(held_x[span, :], up_ref[...], preferred_element_type=jnp.float32)
        back_grad = lax.dot_general(
            held_c[span, :],
            down_ref[...],
            (((1,), (1,)), ((), ())),
            preferred_element_type=jnp.float32,
        )
        squash = jax.nn.sigmoid(preact)
        held_hid[span, :] = (preact * squash).astype(jnp.bfloat16)
        slope = squash * (1.0 + preact * (1.0 - squash))
        held_pre[span, :] = (back_grad * slope).astype(jnp.bfloat16)
        return carry

    lax.fori_loop(0, held_x.shape[0] // tile, rows_of, 0)


def column_sums(left, right):
    return lax.dot_general(left, right, (((0,), (0,)), ((), ())), preferred_element_type=jnp.float32)


def absorb(place, blocks, w_up, w_down, sums):
    arrays = flatten(blocks)
    width, hidden_units = w_up.shape
    total = sum(first.shape[1] for _, first, _ in blocks)
    have = sums is not None
    step = width // 7
    tile = total // 2 if total > 128 else total

    def body(place_ref, *refs):
        ins, refs = refs[: len(arrays)], refs[len(arrays) :]
        up_ref, down_ref = refs[:2]
        refs = refs[2:]
        if have:
            old_up, old_down = refs[:2]
            refs = refs[2:]
        out_up, out_down, held_x, held_c, held_pre, held_hid = refs
        gather_rows(place_ref[0], blocks, ins, held_x, held_c)
        row_terms(up_ref, down_ref, held_x, held_c, held_pre, held_hid, tile)

        def columns(j, carry):
            span = pl.ds(pl.multiple_of(j * step, step), step)
            part_up = column_sums(held_pre[...], held_x[:, span])
            part_down = column_sums(held_hid[...], held_c[:, span])
            out_up[:, span] = part_up + old_up[:, span] if have else part_up
            out_down[:, span] = part_down + old_down[:, span] if have else part_down
            return carry

        lax.fori_loop(0, 7, columns, 0)

    shape = jax.ShapeDtypeStruct((hidden_units, width), jnp.float32)
    args = [place, *arrays, w_up, w_down] + (list(sums) if have else [])
    return pl.pallas_call(
        body,
        out_shape=[shape, shape],
        in_specs=[SMEM] + [VMEM] * (len(args) - 1),
        out_specs=[VMEM, VMEM],
        scratch_shapes=[
            pltpu.VMEM((total, width), jnp.bfloat16),
            pltpu.VMEM((total, width), jnp.bfloat16),
            pltpu.VMEM((total, hidden_units), jnp.bfloat16),
            pltpu.VMEM((total, hidden_units), jnp.bfloat16),
        ],
        input_output_aliases={len(args) - 2: 0, len(args) - 1: 1} if have else {},
        compiler_params=pltpu.CompilerParams(vmem_limit_bytes=LIMIT),
        cost_estimate=pl.CostEstimate(
            flops=8 * total * width * hidden_units,
            transcendentals=0,
            bytes_accessed=4 * total * width,
        ),
        name="absorb",
    )(*args)


def adam_step(gradient, moment_one, moment_two):
    new_one = BETA_ONE * moment_one.astype(jnp.float32) + (1.0 - BETA_ONE) * gradient
    new_two = BETA_TWO * moment_two.astype(jnp.float32) + (1.0 - BETA_TWO) * gradient * gradient
    return new_one / (jnp.sqrt(new_two) + EPSILON)


def finish_down(place, my_index, leaving, tile_owner, blocks, w_up, w_down, old, m_down, v_down):
    arrays = flatten(blocks)
    width, hidden_units = w_up.shape
    tiles = tile_owner.shape[0]
    tile_rows = width // tiles
    total = sum(first.shape[1] for _, first, _ in blocks)
    step = 256

    def body(place_ref, me, leave, owner, *refs):
        ins, refs = refs[: len(arrays)], refs[len(arrays) :]
        up_ref, down_ref, old_down, md, vd = refs[:5]
        out_down, out_tiles, out_x, out_pre, both, held_c, held_hid = refs[5:]
        keep = me[0] != leave[0]
        gather_rows(place_ref[0], blocks, ins, out_x, held_c)
        row_terms(up_ref, down_ref, out_x, held_c, out_pre, held_hid, total)

        def columns(j, carry):
            span = pl.ds(pl.multiple_of(j * step, step), step)
            grad = old_down[:, span] + column_sums(held_hid[...], held_c[:, span])
            step_down = adam_step(grad, md[:, span], vd[:, span])
            both[span, :] = step_down.T.astype(jnp.bfloat16)
            out_down[:, span] = jnp.where(keep, step_down, 0.0).astype(jnp.bfloat16)
            return carry

        lax.fori_loop(0, width // step, columns, 0)
        for t in range(tiles):
            out_tiles[owner[t]] = both[t * tile_rows : (t + 1) * tile_rows, :]

    return pl.pallas_call(
        body,
        out_shape=[
            jax.ShapeDtypeStruct((hidden_units, width), jnp.bfloat16),
            jax.ShapeDtypeStruct((tiles, tile_rows, hidden_units), jnp.bfloat16),
            jax.ShapeDtypeStruct((total, width), jnp.bfloat16),
            jax.ShapeDtypeStruct((total, hidden_units), jnp.bfloat16),
        ],
        in_specs=[SMEM] * 4 + [VMEM] * (len(arrays) + 5),
        out_specs=[VMEM] * 4,
        scratch_shapes=[
            pltpu.VMEM((width, hidden_units), jnp.bfloat16),
            pltpu.VMEM((total, width), jnp.bfloat16),
            pltpu.VMEM((total, hidden_units), jnp.bfloat16),
        ],
        compiler_params=pltpu.CompilerParams(vmem_limit_bytes=LIMIT),
        name="finish_down",
    )(place, my_index, leaving, tile_owner, *arrays, w_up, w_down, old, m_down, v_down)


def finish_up(my_index, leaving, tile_owner, rows_x, pre_grad, old, m_up, v_up):
    width, hidden_units = m_up.shape
    tiles = tile_owner.shape[0]
    tile_rows = width // tiles
    step = 256

    def body(me, leave, owner, x_ref, pre_ref, old_up, mu, vu, out_up, out_tiles, both):
        keep = me[0] != leave[0]

        def columns(j, carry):
            span = pl.ds(pl.multiple_of(j * step, step), step)
            grad = old_up[:, span] + column_sums(pre_ref[...], x_ref[:, span])
            step_up = adam_step(grad.T, mu[span, :], vu[span, :])
            both[span, :] = step_up.astype(jnp.bfloat16)
            out_up[span, :] = jnp.where(keep, step_up, 0.0).astype(jnp.bfloat16)
            return carry

        lax.fori_loop(0, width // step, columns, 0)
        for t in range(tiles):
            out_tiles[owner[t]] = both[t * tile_rows : (t + 1) * tile_rows, :]

    return pl.pallas_call(
        body,
        out_shape=[
            jax.ShapeDtypeStruct((width, hidden_units), jnp.bfloat16),
            jax.ShapeDtypeStruct((tiles, tile_rows, hidden_units), jnp.bfloat16),
        ],
        in_specs=[SMEM] * 3 + [VMEM] * 5,
        out_specs=[VMEM] * 2,
        scratch_shapes=[pltpu.VMEM((width, hidden_units), jnp.bfloat16)],
        compiler_params=pltpu.CompilerParams(vmem_limit_bytes=LIMIT),
        cost_estimate=pl.CostEstimate(
            flops=8 * 160 * width * hidden_units,
            transcendentals=0,
            bytes_accessed=12 * width * hidden_units,
        ),
        name="finish_up",
    )(my_index, leaving, tile_owner, rows_x, pre_grad, old, m_up, v_up)


def on_device(
    tokens, cotangent, gates, routes, w_up, w_down, m_up, v_up, m_down, v_down, leaving, tile_owner
):
    tok_count, width = tokens.shape
    piece = width // PIECES
    core = lax.axis_index("co")
    low = lax.axis_index("zl")
    half = lax.axis_index("zh")
    column = lax.axis_index(("y", "x"))
    place = jnp.where(core == 0, low, 3 - low)
    base = jnp.where(low <= 1, half, 1 - half)
    place_ref = place.reshape(1)

    outgoing = prepare(
        base.reshape(1),
        tokens,
        cotangent,
        gates.reshape(1, tok_count),
        routes.reshape(1, tok_count),
        SLOT_GROUPS,
    )

    def step(value, places):
        return lax.ppermute(value, ALL, stream_pairs(places))

    def swap(value):
        return lax.ppermute(value, ALL, swap_pairs())

    chunks = []
    previous = None
    for tag, (_, slots), sent in zip(TAGS, SLOT_GROUPS, outgoing):
        rows = sent.shape[0]
        if previous is not None:
            previous, sent = lax.optimization_barrier((previous, sent))
            chunks[-1][0] = previous
        previous = lax.all_to_all(
            sent.reshape(32, rows // 32, piece), ("co", "y", "x"), 0, 0, tiled=True
        ).reshape(rows, piece)
        chunks.append({"tag": tag, "slots": slots, 0: previous})
    everyone = (0, 1, 2, 3)
    for ch in chunks:
        tag = ch["tag"]
        ch[0] = arrange(ch[0], ch["slots"])
        ch[1] = step(ch[0], everyone)
        ch["s0"] = swap(ch[0])
        ch[2] = step(jnp.where(place == 2, ch["s0"], ch[1]), everyone)
        ch["s1"] = swap(ch[1])
        ch[3] = step(jnp.where(place == 2, ch[1], ch[2]), (0, 1, 2))
        ch["s2"] = swap(ch[2])
        ch[4] = step(jnp.where(place == 2, ch[2], ch[3]), (1, 2))
        ch["s3"] = swap(ch[3])
        ch[5] = step(ch[3], (2,))
        ch["s4"] = swap(ch[4])
        ch[6] = step(ch[4], (2,))
        ch["s5"] = swap(ch[5])
        ch["s6"] = swap(ch[6])

    rules = {
        "o": (lambda at: at <= 1, 0, "s0"),
        "1": (lambda at: at < 3, 1, None),
        "p": (lambda at: at > 0, "s1", None),
        "2": (None, 2, None),
        "q": (None, "s2", None),
        "3": (None, 3, None),
        "r": (None, "s3", None),
        "4": (lambda at: at >= 2, 4, "s4"),
        "5": (lambda at: at == 3, 5, "s5"),
        "6": (lambda at: at == 3, 6, "s6"),
    }

    def blocks_of(words):
        blocks = []
        for word in words.split():
            ch = chunks[TAGS.index(word[0])]
            for letter in word[1:]:
                test, one, two = rules[letter]
                blocks.append((test, ch[one], None if two is None else ch[two]))
        return blocks

    sums = None
    for words in SUMS:
        sums = absorb(place_ref, blocks_of(words), w_up[0], w_down[0], sums)
    my_index = (column * 2 + half).reshape(1)
    leaver = leaving[0]

    def adopt(tiles):
        _, rows, units = tiles.shape
        incoming = lax.all_to_all(tiles.reshape(16, 2, rows, units), ("y", "x"), 0, 0, tiled=True)
        pair = lax.dynamic_index_in_dim(incoming, leaver // 2, 0, keepdims=False)
        own = lax.dynamic_index_in_dim(pair, half, 0, keepdims=False)
        other = lax.dynamic_index_in_dim(pair, 1 - half, 0, keepdims=False)
        crossed = lax.ppermute(other, ALL, across_pairs())
        return jnp.where(half == leaver % 2, own, crossed)[None]

    update_down, tiles_down, rows_x, pre_grad = finish_down(
        place_ref,
        my_index,
        leaving,
        tile_owner,
        blocks_of(LAST),
        w_up[0],
        w_down[0],
        sums[1],
        m_down[0],
        v_down[0],
    )
    adopted_down = adopt(tiles_down)
    update_up, tiles_up = finish_up(
        my_index, leaving, tile_owner, rows_x, pre_grad, sums[0], m_up[0], v_up[0]
    )
    adopted_up = adopt(tiles_up)
    return (update_up[None], update_down[None], adopted_up, adopted_down)


def solution(mesh):
    wide = Mesh(mesh.devices.reshape(4, 2, 4, 4, 2), ALL)
    dp = ("zl", "co")
    expert = ("y", "x", "zh")
    row = P(dp + expert, None)
    up = P(expert, None, dp)
    down = P(expert, dp, None)
    return jax.shard_map(
        on_device,
        mesh=wide,
        in_specs=(row, row, row, row, up, down, up, up, down, down, P(), P()),
        out_specs=(up, down, up, up),
        check_vma=False,
    )
```

```python
import jax
import jax.numpy as jnp
from jax import lax
from jax.experimental import pallas as pl
from jax.experimental.pallas import tpu as pltpu
from jax.sharding import Mesh
from jax.sharding import PartitionSpec as P


BETA_ONE = 0.9
BETA_TWO = 0.95
EPSILON = 1e-08

ALL = ("zl", "co", "y", "x", "zh")
SLOT_GROUPS = ((0, 2), (2, 3))
TAGS = ("a", "b")
SUMS = ("ao1p2q3r", "a4 bo1p", "a5 b2q", "a6 b3r", "b45")
LAST = "b6"
PIECES = 4
VMEM = pl.BlockSpec(memory_space=pltpu.VMEM)
SMEM = pl.BlockSpec(memory_space=pltpu.SMEM)
HBM = pl.BlockSpec(memory_space=pltpu.MemorySpace.HBM)
LIMIT = 60 * 1024 * 1024


def device_id(z, core, y, x):
    return (((z % 4) * 2 + core) * 4 + y) * 8 + x * 2 + z // 4


def every():
    for z in range(8):
        for core in range(2):
            for y in range(4):
                for x in range(4):
                    yield z, core, y, x


def stream_pairs(places):
    pairs = []
    for z, core, y, x in every():
        place = z % 4 if core == 0 else 3 - z % 4
        if place in places:
            there = (z + (1 if core == 0 else -1)) % 8
            pairs.append((device_id(z, core, y, x), device_id(there, core, y, x)))
    return pairs


def swap_pairs():
    return [(device_id(z, c, y, x), device_id(z, 1 - c, y, x)) for z, c, y, x in every()]


def across_pairs():
    return [(device_id(z, c, y, x), device_id((z + 4) % 8, c, y, x)) for z, c, y, x in every()]


def over(value, divisor):
    if divisor & (divisor - 1) == 0:
        return value >> (divisor.bit_length() - 1)
    return (value * (-(-(1 << 18) // divisor))) >> 18


def prepare(base, tokens, cotangent, gates_row, routes_row, outs_slots):
    tok_count, width = tokens.shape
    piece = width // PIECES
    parts = 2 * PIECES

    def body(base_ref, x_ref, c_ref, g_ref, r_ref, *rest):
        outs, (held,) = rest[:-1], rest[-1:]
        routes = jnp.broadcast_to(r_ref[...], (tok_count, tok_count))
        routes_down = routes.T
        gate_down = jnp.broadcast_to(g_ref[...], (tok_count, tok_count)).T
        at_row = lax.broadcasted_iota(jnp.int32, (tok_count, tok_count), 0)
        at_col = lax.broadcasted_iota(jnp.int32, (tok_count, tok_count), 1)
        before = jnp.where((routes_down == routes) & (at_row < at_col), 1, 0)
        rank = jnp.sum(before, axis=0, keepdims=True)
        code = r_ref[...] * 8 + rank
        for q in range(PIECES):
            held[q * tok_count : (q + 1) * tok_count, :] = x_ref[:, q * piece : (q + 1) * piece]
            for j in range(piece // 128):
                cols = c_ref[:, q * piece + j * 128 : q * piece + (j + 1) * 128]
                held[
                    (PIECES + q) * tok_count : (PIECES + q + 1) * tok_count,
                    j * 128 : (j + 1) * 128,
                ] = (gate_down * cols.astype(jnp.float32)).astype(jnp.bfloat16)
        for out, (first, slots) in zip(outs, outs_slots):
            rows = 32 * parts * slots
            row = lax.broadcasted_iota(jnp.int32, (rows, tok_count), 0)
            group = over(row, slots)
            slot = row - group * slots
            part = group & (parts - 1)
            dest = group >> 3
            expert = ((dest & 15) << 1) | (base_ref[0] ^ (dest >> 4))
            hit = (expert * 8 + (slot + first)) == code
            picker = jnp.concatenate(
                [
                    jnp.where(hit & (part == q), 1.0, 0.0).astype(jnp.bfloat16)
                    for q in range(parts)
                ],
                axis=1,
            )
            out[...] = jnp.dot(
                picker, held[...], preferred_element_type=jnp.float32
            ).astype(jnp.bfloat16)

    return pl.pallas_call(
        body,
        out_shape=[
            jax.ShapeDtypeStruct((32 * parts * slots, piece), jnp.bfloat16)
            for _, slots in outs_slots
        ],
        in_specs=[SMEM, VMEM, VMEM, VMEM, VMEM],
        out_specs=[VMEM] * len(outs_slots),
        scratch_shapes=[pltpu.VMEM((parts * tok_count, piece), jnp.bfloat16)],
        compiler_params=pltpu.CompilerParams(vmem_limit_bytes=LIMIT),
        name="prepare",
    )(base, tokens, cotangent, gates_row, routes_row)


def sorter(slots):
    rows = 16 * 8 * slots
    row = lax.broadcasted_iota(jnp.int32, (rows, rows), 0)
    col = lax.broadcasted_iota(jnp.int32, (rows, rows), 1)
    part = over(row, 16 * slots)
    rest = row - part * (16 * slots)
    sender = over(rest, slots)
    slot = rest - sender * slots
    return jnp.where(col == sender * (8 * slots) + part * slots + slot, 1.0, 0.0).astype(
        jnp.bfloat16
    )


def arrange(received, slots):
    _, piece = received.shape
    count = 16 * slots

    def body(in_ref, out_ref):
        order = sorter(slots)
        for half in range(2):
            block = in_ref[half * 8 * count : (half + 1) * 8 * count, :]
            ordered = jnp.dot(order, block, preferred_element_type=jnp.float32)
            ordered = ordered.astype(jnp.bfloat16)
            for q in range(2 * PIECES):
                out_ref[q, half * count : (half + 1) * count, :] = ordered[
                    q * count : (q + 1) * count, :
                ]

    return pl.pallas_call(
        body,
        out_shape=jax.ShapeDtypeStruct((2 * PIECES, 2 * count, piece), jnp.bfloat16),
        in_specs=[VMEM],
        out_specs=VMEM,
        compiler_params=pltpu.CompilerParams(vmem_limit_bytes=LIMIT),
        name="arrange",
    )(received)


def flatten(blocks):
    arrays = []
    for _, first, second in blocks:
        arrays.append(first)
        if second is not None:
            arrays.append(second)
    return arrays


def gather_rows(at, blocks, refs, held_x, held_c):
    refs = list(refs)
    piece = refs[0].shape[2]
    offset = 0
    for test, _, second in blocks:
        first_ref = refs.pop(0)
        second_ref = refs.pop(0) if second is not None else None
        count = first_ref.shape[1]
        for q in range(2 * PIECES):
            part = first_ref[q]
            if second_ref is not None:
                part = jnp.where(test(at), part, second_ref[q])
            elif test is not None and q >= PIECES:
                part = jnp.where(test(at), part, jnp.zeros_like(part))
            held = held_x if q < PIECES else held_c
            left = (q % PIECES) * piece
            held[offset : offset + count, left : left + piece] = part
        offset += count


def row_terms(up_ref, down_ref, held_x, held_c, held_pre, held_hid, tile):
    def rows_of(i, carry):
        span = pl.ds(pl.multiple_of(i * tile, tile), tile)
        preact = jnp.dot(held_x[span, :], up_ref[...], preferred_element_type=jnp.float32)
        back_grad = lax.dot_general(
            held_c[span, :],
            down_ref[...],
            (((1,), (1,)), ((), ())),
            preferred_element_type=jnp.float32,
        )
        squash = jax.nn.sigmoid(preact)
        held_hid[span, :] = (preact * squash).astype(jnp.bfloat16)
        slope = squash * (1.0 + preact * (1.0 - squash))
        held_pre[span, :] = (back_grad * slope).astype(jnp.bfloat16)
        return carry

    lax.fori_loop(0, held_x.shape[0] // tile, rows_of, 0)


def column_sums(left, right):
    return lax.dot_general(left, right, (((0,), (0,)), ((), ())), preferred_element_type=jnp.float32)


def absorb(place, blocks, w_up, w_down, sums):
    arrays = flatten(blocks)
    width, hidden_units = w_up.shape
    total = sum(first.shape[1] for _, first, _ in blocks)
    have = sums is not None
    steps = 7
    step = width // steps
    tile = total // 2 if total > 128 else total
    count = len(arrays)

    def body(place_ref, *refs):
        hbm_in, refs = refs[: count + 2], refs[count + 2 :]
        if have:
            hbm_in, refs = hbm_in + refs[:2], refs[2:]
        outs, refs = refs[:2], refs[2:]
        vmem_in, refs = list(refs[: count + 2]), refs[count + 2 :]
        acc_up, acc_down, held_x, held_c, held_pre, held_hid, in_sems, out_sems = refs
        if have:
            vmem_in += [acc_up, acc_down]
        copies = [
            pltpu.make_async_copy(source, target, in_sems.at[i])
            for i, (source, target) in enumerate(zip(hbm_in, vmem_in))
        ]
        for copy in copies:
            copy.start()
        for copy in copies[:count]:
            copy.wait()
        gather_rows(place_ref[0], blocks, vmem_in[:count], held_x, held_c)
        for copy in copies[count : count + 2]:
            copy.wait()
        row_terms(vmem_in[count], vmem_in[count + 1], held_x, held_c, held_pre, held_hid, tile)
        for copy in copies[count + 2 :]:
            copy.wait()

        def leave(j):
            span = pl.ds(pl.multiple_of(j * step, step), step)
            return [
                pltpu.make_async_copy(acc.at[:, span], out.at[:, span], out_sems.at[k, j])
                for k, (acc, out) in enumerate(zip((acc_up, acc_down), outs))
            ]

        def columns(j, carry):
            span = pl.ds(pl.multiple_of(j * step, step), step)
            part_up = column_sums(held_pre[...], held_x[:, span])
            acc_up[:, span] = part_up + acc_up[:, span] if have else part_up
            part_down = column_sums(held_hid[...], held_c[:, span])
            acc_down[:, span] = part_down + acc_down[:, span] if have else part_down
            for copy in leave(j):
                copy.start()
            return carry

        def drain(j, carry):
            for copy in leave(j):
                copy.wait()
            return carry

        lax.fori_loop(0, steps, columns, 0)
        lax.fori_loop(0, steps, drain, 0)

    shape = jax.ShapeDtypeStruct((hidden_units, width), jnp.float32)
    args = [place, *arrays, w_up, w_down] + (list(sums) if have else [])
    return pl.pallas_call(
        body,
        out_shape=[shape, shape],
        in_specs=[SMEM] + [HBM] * (len(args) - 1),
        out_specs=[HBM, HBM],
        scratch_shapes=[pltpu.VMEM(a.shape, a.dtype) for a in (*arrays, w_up, w_down)]
        + [
            pltpu.VMEM((hidden_units, width), jnp.float32),
            pltpu.VMEM((hidden_units, width), jnp.float32),
            pltpu.VMEM((total, width), jnp.bfloat16),
            pltpu.VMEM((total, width), jnp.bfloat16),
            pltpu.VMEM((total, hidden_units), jnp.bfloat16),
            pltpu.VMEM((total, hidden_units), jnp.bfloat16),
            pltpu.SemaphoreType.DMA((len(args) - 1,)),
            pltpu.SemaphoreType.DMA((2, steps)),
        ],
        input_output_aliases={len(args) - 2: 0, len(args) - 1: 1} if have else {},
        compiler_params=pltpu.CompilerParams(vmem_limit_bytes=LIMIT),
        cost_estimate=pl.CostEstimate(
            flops=8 * total * width * hidden_units,
            transcendentals=0,
            bytes_accessed=4 * total * width,
        ),
        name="absorb",
    )(*args)


def adam_step(gradient, moment_one, moment_two):
    new_one = BETA_ONE * moment_one.astype(jnp.float32) + (1.0 - BETA_ONE) * gradient
    new_two = BETA_TWO * moment_two.astype(jnp.float32) + (1.0 - BETA_TWO) * gradient * gradient
    return new_one / (jnp.sqrt(new_two) + EPSILON)


def finish_down(place, my_index, leaving, tile_owner, blocks, w_up, w_down, old, m_down, v_down):
    arrays = flatten(blocks)
    width, hidden_units = w_up.shape
    tiles = tile_owner.shape[0]
    tile_rows = width // tiles
    total = sum(first.shape[1] for _, first, _ in blocks)
    step = width // PIECES

    count = len(arrays)

    def body(place_ref, me, leave, owner, *refs):
        hbm_in, refs = refs[: count + 5], refs[count + 5 :]
        out_down, out_tiles, out_x, out_pre = refs[:4]
        vmem_in, refs = refs[4 : count + 9], refs[count + 9 :]
        both, held_c, held_hid, sems = refs
        copies = [
            pltpu.make_async_copy(source, target, sems.at[i])
            for i, (source, target) in enumerate(zip(hbm_in, vmem_in))
        ]
        for copy in copies:
            copy.start()
        keep = me[0] != leave[0]
        for copy in copies[:count]:
            copy.wait()
        gather_rows(place_ref[0], blocks, vmem_in[:count], out_x, held_c)
        up_ref, down_ref, old_down, md, vd = vmem_in[count:]
        for copy in copies[count : count + 2]:
            copy.wait()
        row_terms(up_ref, down_ref, out_x, held_c, out_pre, held_hid, total)
        for copy in copies[count + 2 :]:
            copy.wait()

        def columns(j, carry):
            span = pl.ds(pl.multiple_of(j * step, step), step)
            grad = old_down[:, span] + column_sums(held_hid[...], held_c[:, span])
            step_down = adam_step(grad, md[:, span], vd[:, span])
            both[span, :] = step_down.T.astype(jnp.bfloat16)
            out_down[:, span] = jnp.where(keep, step_down, 0.0).astype(jnp.bfloat16)
            return carry

        lax.fori_loop(0, width // step, columns, 0)
        for t in range(tiles):
            out_tiles[owner[t]] = both[t * tile_rows : (t + 1) * tile_rows, :]

    args = (*arrays, w_up, w_down, old, m_down, v_down)
    return pl.pallas_call(
        body,
        out_shape=[
            jax.ShapeDtypeStruct((hidden_units, width), jnp.bfloat16),
            jax.ShapeDtypeStruct((tiles, tile_rows, hidden_units), jnp.bfloat16),
            jax.ShapeDtypeStruct((total, width), jnp.bfloat16),
            jax.ShapeDtypeStruct((total, hidden_units), jnp.bfloat16),
        ],
        in_specs=[SMEM] * 4 + [HBM] * len(args),
        out_specs=[VMEM] * 4,
        scratch_shapes=[pltpu.VMEM(a.shape, a.dtype) for a in args]
        + [
            pltpu.VMEM((width, hidden_units), jnp.bfloat16),
            pltpu.VMEM((total, width), jnp.bfloat16),
            pltpu.VMEM((total, hidden_units), jnp.bfloat16),
            pltpu.SemaphoreType.DMA((len(args),)),
        ],
        compiler_params=pltpu.CompilerParams(vmem_limit_bytes=LIMIT),
        name="finish_down",
    )(place, my_index, leaving, tile_owner, *args)


def finish_up(my_index, leaving, tile_owner, rows_x, pre_grad, old, m_up, v_up):
    width, hidden_units = m_up.shape
    tiles = tile_owner.shape[0]
    tile_rows = width // tiles
    step = width // PIECES

    def body(me, leave, owner, x_ref, pre_ref, old_up, mu, vu, out_up, out_tiles, both):
        keep = me[0] != leave[0]

        def columns(j, carry):
            span = pl.ds(pl.multiple_of(j * step, step), step)
            grad = old_up[:, span] + column_sums(pre_ref[...], x_ref[:, span])
            step_up = adam_step(grad.T, mu[span, :], vu[span, :])
            both[span, :] = step_up.astype(jnp.bfloat16)
            out_up[span, :] = jnp.where(keep, step_up, 0.0).astype(jnp.bfloat16)
            return carry

        lax.fori_loop(0, width // step, columns, 0)
        for t in range(tiles):
            out_tiles[owner[t]] = both[t * tile_rows : (t + 1) * tile_rows, :]

    return pl.pallas_call(
        body,
        out_shape=[
            jax.ShapeDtypeStruct((width, hidden_units), jnp.bfloat16),
            jax.ShapeDtypeStruct((tiles, tile_rows, hidden_units), jnp.bfloat16),
        ],
        in_specs=[SMEM] * 3 + [VMEM] * 5,
        out_specs=[VMEM] * 2,
        scratch_shapes=[pltpu.VMEM((width, hidden_units), jnp.bfloat16)],
        compiler_params=pltpu.CompilerParams(vmem_limit_bytes=LIMIT),
        cost_estimate=pl.CostEstimate(
            flops=8 * 160 * width * hidden_units,
            transcendentals=0,
            bytes_accessed=12 * width * hidden_units,
        ),
        name="finish_up",
    )(my_index, leaving, tile_owner, rows_x, pre_grad, old, m_up, v_up)


def on_device(
    tokens, cotangent, gates, routes, w_up, w_down, m_up, v_up, m_down, v_down, leaving, tile_owner
):
    tok_count, width = tokens.shape
    piece = width // PIECES
    core = lax.axis_index("co")
    low = lax.axis_index("zl")
    half = lax.axis_index("zh")
    column = lax.axis_index(("y", "x"))
    place = jnp.where(core == 0, low, 3 - low)
    base = jnp.where(low <= 1, half, 1 - half)
    place_ref = place.reshape(1)

    outgoing = []
    for tag, group in zip(TAGS, SLOT_GROUPS):
        outgoing += prepare(
            base.reshape(1),
            tokens,
            cotangent,
            gates.reshape(1, tok_count),
            routes.reshape(1, tok_count),
            (group,),
        )

    def step(value, places):
        return lax.ppermute(value, ALL, stream_pairs(places))

    def swap(value):
        return lax.ppermute(value, ALL, swap_pairs())

    chunks = []
    previous = None
    for tag, (_, slots), sent in zip(TAGS, SLOT_GROUPS, outgoing):
        rows = sent.shape[0]
        if previous is not None:
            previous, sent = lax.optimization_barrier((previous, sent))
            chunks[-1][0] = previous
        previous = lax.all_to_all(
            sent.reshape(32, rows // 32, piece), ("co", "y", "x"), 0, 0, tiled=True
        ).reshape(rows, piece)
        chunks.append({"tag": tag, "slots": slots, 0: previous})

    def joined(first, second):
        return jnp.where(place == 3, first, second)

    for ch in chunks:
        tag = ch["tag"]
        ch[0] = arrange(ch[0], ch["slots"])
        ch[1] = step(ch[0], (0, 1, 2, 3))
        ch["s0"] = swap(ch[0])
        x2 = step(ch["s0"], (2,))
        y2 = step(ch[1], (0, 1, 3))
        ch["s1"] = swap(ch[1])
        x3 = step(ch[1], (2,))
        y3 = step(y2, (0, 1))
        ch[2] = joined(x2, y2)
        ch["s2"] = swap(ch[2])
        x4 = step(y2, (2,))
        y4 = step(y3, (1,))
        ch[3] = joined(x3, y3)
        ch["s3"] = swap(ch[3])
        ch[5] = step(y3, (2,))
        ch[4] = joined(x4, y4)
        ch["s4"] = swap(ch[4])
        ch[6] = step(y4, (2,))
        ch["s5"] = swap(ch[5])
        ch["s6"] = swap(ch[6])

    rules = {
        "o": (lambda at: at <= 1, 0, "s0"),
        "1": (lambda at: at < 3, 1, None),
        "p": (lambda at: at > 0, "s1", None),
        "2": (None, 2, None),
        "q": (None, "s2", None),
        "3": (None, 3, None),
        "r": (None, "s3", None),
        "4": (lambda at: at >= 2, 4, "s4"),
        "5": (lambda at: at == 3, 5, "s5"),
        "6": (lambda at: at == 3, 6, "s6"),
    }

    def blocks_of(words):
        blocks = []
        for word in words.split():
            ch = chunks[TAGS.index(word[0])]
            for letter in word[1:]:
                test, one, two = rules[letter]
                blocks.append((test, ch[one], None if two is None else ch[two]))
        return blocks

    sums = None
    for words in SUMS:
        sums = absorb(place_ref, blocks_of(words), w_up[0], w_down[0], sums)
    my_index = (column * 2 + half).reshape(1)
    leaver = leaving[0]

    def adopt(tiles):
        _, rows, units = tiles.shape
        incoming = lax.all_to_all(tiles.reshape(16, 2, rows, units), ("y", "x"), 0, 0, tiled=True)
        pair = lax.dynamic_index_in_dim(incoming, leaver // 2, 0, keepdims=False)
        own = lax.dynamic_index_in_dim(pair, half, 0, keepdims=False)
        other = lax.dynamic_index_in_dim(pair, 1 - half, 0, keepdims=False)
        crossed = lax.ppermute(other, ALL, across_pairs())
        return jnp.where(half == leaver % 2, own, crossed)[None]

    update_down, tiles_down, rows_x, pre_grad = finish_down(
        place_ref,
        my_index,
        leaving,
        tile_owner,
        blocks_of(LAST),
        w_up[0],
        w_down[0],
        sums[1],
        m_down[0],
        v_down[0],
    )
    adopted_down = adopt(tiles_down)
    update_up, tiles_up = finish_up(
        my_index, leaving, tile_owner, rows_x, pre_grad, sums[0], m_up[0], v_up[0]
    )
    adopted_up = adopt(tiles_up)
    return (update_up[None], update_down[None], adopted_up, adopted_down)


def solution(mesh):
    wide = Mesh(mesh.devices.reshape(4, 2, 4, 4, 2), ALL)
    dp = ("zl", "co")
    expert = ("y", "x", "zh")
    row = P(dp + expert, None)
    up = P(expert, None, dp)
    down = P(expert, dp, None)
    return jax.shard_map(
        on_device,
        mesh=wide,
        in_specs=(row, row, row, row, up, down, up, up, down, down, P(), P()),
        out_specs=(up, down, up, up),
        check_vma=False,
    )
```

```python
import jax
import jax.numpy as jnp
from jax import lax
from jax.experimental import pallas as pl
from jax.experimental.pallas import tpu as pltpu
from jax.sharding import Mesh
from jax.sharding import PartitionSpec as P


BETA_ONE = 0.9
BETA_TWO = 0.95
EPSILON = 1e-08

ALL = ("zl", "co", "y", "x", "zh")
SLOT_GROUPS = ((0, 2), (2, 3))
TAGS = ("a", "b")
SUMS = ("ao1p2q3r", "a4 bo1p", "a5 b2q", "a6 b3r4")
LAST = "b56"
PIECES = 4
VMEM = pl.BlockSpec(memory_space=pltpu.VMEM)
SMEM = pl.BlockSpec(memory_space=pltpu.SMEM)
HBM = pl.BlockSpec(memory_space=pltpu.MemorySpace.HBM)
LIMIT = 60 * 1024 * 1024


def device_id(z, core, y, x):
    return (((z % 4) * 2 + core) * 4 + y) * 8 + x * 2 + z // 4


def every():
    for z in range(8):
        for core in range(2):
            for y in range(4):
                for x in range(4):
                    yield z, core, y, x


def stream_pairs(places):
    pairs = []
    for z, core, y, x in every():
        place = z % 4 if core == 0 else 3 - z % 4
        if place in places:
            there = (z + (1 if core == 0 else -1)) % 8
            pairs.append((device_id(z, core, y, x), device_id(there, core, y, x)))
    return pairs


def swap_pairs():
    return [(device_id(z, c, y, x), device_id(z, 1 - c, y, x)) for z, c, y, x in every()]


def across_pairs():
    return [(device_id(z, c, y, x), device_id((z + 4) % 8, c, y, x)) for z, c, y, x in every()]


def over(value, divisor):
    if divisor & (divisor - 1) == 0:
        return value >> (divisor.bit_length() - 1)
    return (value * (-(-(1 << 18) // divisor))) >> 18


def prepare(base, tokens, cotangent, gates_row, routes_row, outs_slots):
    tok_count, width = tokens.shape
    piece = width // PIECES
    parts = 2 * PIECES

    def body(base_ref, x_ref, c_ref, g_ref, r_ref, *rest):
        outs, (held,) = rest[:-1], rest[-1:]
        routes = jnp.broadcast_to(r_ref[...], (tok_count, tok_count))
        routes_down = routes.T
        gate_down = jnp.broadcast_to(g_ref[...], (tok_count, tok_count)).T
        at_row = lax.broadcasted_iota(jnp.int32, (tok_count, tok_count), 0)
        at_col = lax.broadcasted_iota(jnp.int32, (tok_count, tok_count), 1)
        before = jnp.where((routes_down == routes) & (at_row < at_col), 1, 0)
        rank = jnp.sum(before, axis=0, keepdims=True)
        code = r_ref[...] * 8 + rank
        for q in range(PIECES):
            held[q * tok_count : (q + 1) * tok_count, :] = x_ref[:, q * piece : (q + 1) * piece]
            for j in range(piece // 128):
                cols = c_ref[:, q * piece + j * 128 : q * piece + (j + 1) * 128]
                held[
                    (PIECES + q) * tok_count : (PIECES + q + 1) * tok_count,
                    j * 128 : (j + 1) * 128,
                ] = (gate_down * cols.astype(jnp.float32)).astype(jnp.bfloat16)
        for out, (first, slots) in zip(outs, outs_slots):
            rows = 32 * parts * slots
            row = lax.broadcasted_iota(jnp.int32, (rows, tok_count), 0)
            group = over(row, slots)
            slot = row - group * slots
            part = group & (parts - 1)
            dest = group >> 3
            expert = ((dest & 15) << 1) | (base_ref[0] ^ (dest >> 4))
            hit = (expert * 8 + (slot + first)) == code
            picker = jnp.concatenate(
                [
                    jnp.where(hit & (part == q), 1.0, 0.0).astype(jnp.bfloat16)
                    for q in range(parts)
                ],
                axis=1,
            )
            out[...] = jnp.dot(
                picker, held[...], preferred_element_type=jnp.float32
            ).astype(jnp.bfloat16)

    return pl.pallas_call(
        body,
        out_shape=[
            jax.ShapeDtypeStruct((32 * parts * slots, piece), jnp.bfloat16)
            for _, slots in outs_slots
        ],
        in_specs=[SMEM, VMEM, VMEM, VMEM, VMEM],
        out_specs=[VMEM] * len(outs_slots),
        scratch_shapes=[pltpu.VMEM((parts * tok_count, piece), jnp.bfloat16)],
        compiler_params=pltpu.CompilerParams(vmem_limit_bytes=LIMIT),
        name="prepare",
    )(base, tokens, cotangent, gates_row, routes_row)


def sorter(slots):
    rows = 16 * 8 * slots
    row = lax.broadcasted_iota(jnp.int32, (rows, rows), 0)
    col = lax.broadcasted_iota(jnp.int32, (rows, rows), 1)
    part = over(row, 16 * slots)
    rest = row - part * (16 * slots)
    sender = over(rest, slots)
    slot = rest - sender * slots
    return jnp.where(col == sender * (8 * slots) + part * slots + slot, 1.0, 0.0).astype(
        jnp.bfloat16
    )


def arrange(received, slots):
    _, piece = received.shape
    count = 16 * slots

    def body(in_ref, out_ref):
        order = sorter(slots)
        for half in range(2):
            block = in_ref[half * 8 * count : (half + 1) * 8 * count, :]
            ordered = jnp.dot(order, block, preferred_element_type=jnp.float32)
            ordered = ordered.astype(jnp.bfloat16)
            for q in range(2 * PIECES):
                out_ref[q, half * count : (half + 1) * count, :] = ordered[
                    q * count : (q + 1) * count, :
                ]

    return pl.pallas_call(
        body,
        out_shape=jax.ShapeDtypeStruct((2 * PIECES, 2 * count, piece), jnp.bfloat16),
        in_specs=[VMEM],
        out_specs=VMEM,
        compiler_params=pltpu.CompilerParams(vmem_limit_bytes=LIMIT),
        name="arrange",
    )(received)


def flatten(blocks):
    arrays = []
    for _, first, second in blocks:
        arrays.append(first)
        if second is not None:
            arrays.append(second)
    return arrays


def gather_rows(at, blocks, refs, held_x, held_c):
    refs = list(refs)
    piece = refs[0].shape[2]
    offset = 0
    for test, _, second in blocks:
        first_ref = refs.pop(0)
        second_ref = refs.pop(0) if second is not None else None
        count = first_ref.shape[1]
        for q in range(2 * PIECES):
            part = first_ref[q]
            if second_ref is not None:
                part = jnp.where(test(at), part, second_ref[q])
            elif test is not None and q >= PIECES:
                part = jnp.where(test(at), part, jnp.zeros_like(part))
            held = held_x if q < PIECES else held_c
            left = (q % PIECES) * piece
            held[offset : offset + count, left : left + piece] = part
        offset += count


def row_terms(up_ref, down_ref, held_x, held_c, held_pre, held_hid, tile):
    def rows_of(i, carry):
        span = pl.ds(pl.multiple_of(i * tile, tile), tile)
        preact = jnp.dot(held_x[span, :], up_ref[...], preferred_element_type=jnp.float32)
        back_grad = lax.dot_general(
            held_c[span, :],
            down_ref[...],
            (((1,), (1,)), ((), ())),
            preferred_element_type=jnp.float32,
        )
        squash = jax.nn.sigmoid(preact)
        held_hid[span, :] = (preact * squash).astype(jnp.bfloat16)
        slope = squash * (1.0 + preact * (1.0 - squash))
        held_pre[span, :] = (back_grad * slope).astype(jnp.bfloat16)
        return carry

    lax.fori_loop(0, held_x.shape[0] // tile, rows_of, 0)


def column_sums(left, right):
    return lax.dot_general(left, right, (((0,), (0,)), ((), ())), preferred_element_type=jnp.float32)


def absorb(place, blocks, w_up, w_down, sums):
    arrays = flatten(blocks)
    width, hidden_units = w_up.shape
    total = sum(first.shape[1] for _, first, _ in blocks)
    have = sums is not None
    steps = 7
    step = width // steps
    tile = total // 2 if total > 128 else total
    count = len(arrays)

    def body(place_ref, *refs):
        hbm_in, refs = refs[: count + 2], refs[count + 2 :]
        if have:
            hbm_in, refs = hbm_in + refs[:2], refs[2:]
        outs, refs = refs[:2], refs[2:]
        vmem_in, refs = list(refs[: count + 2]), refs[count + 2 :]
        acc_up, acc_down, held_x, held_c, held_pre, held_hid, in_sems, out_sems = refs
        if have:
            vmem_in += [acc_up, acc_down]
        copies = [
            pltpu.make_async_copy(source, target, in_sems.at[i])
            for i, (source, target) in enumerate(zip(hbm_in, vmem_in))
        ]
        for copy in copies:
            copy.start()
        for copy in copies[:count]:
            copy.wait()
        gather_rows(place_ref[0], blocks, vmem_in[:count], held_x, held_c)
        for copy in copies[count : count + 2]:
            copy.wait()
        row_terms(vmem_in[count], vmem_in[count + 1], held_x, held_c, held_pre, held_hid, tile)
        for copy in copies[count + 2 :]:
            copy.wait()

        def leave(j):
            span = pl.ds(pl.multiple_of(j * step, step), step)
            return [
                pltpu.make_async_copy(acc.at[:, span], out.at[:, span], out_sems.at[k, j])
                for k, (acc, out) in enumerate(zip((acc_up, acc_down), outs))
            ]

        def columns(j, carry):
            span = pl.ds(pl.multiple_of(j * step, step), step)
            part_up = column_sums(held_pre[...], held_x[:, span])
            acc_up[:, span] = part_up + acc_up[:, span] if have else part_up
            part_down = column_sums(held_hid[...], held_c[:, span])
            acc_down[:, span] = part_down + acc_down[:, span] if have else part_down
            for copy in leave(j):
                copy.start()
            return carry

        def drain(j, carry):
            for copy in leave(j):
                copy.wait()
            return carry

        lax.fori_loop(0, steps, columns, 0)
        lax.fori_loop(0, steps, drain, 0)

    shape = jax.ShapeDtypeStruct((hidden_units, width), jnp.float32)
    args = [place, *arrays, w_up, w_down] + (list(sums) if have else [])
    return pl.pallas_call(
        body,
        out_shape=[shape, shape],
        in_specs=[SMEM] + [HBM] * (len(args) - 1),
        out_specs=[HBM, HBM],
        scratch_shapes=[pltpu.VMEM(a.shape, a.dtype) for a in (*arrays, w_up, w_down)]
        + [
            pltpu.VMEM((hidden_units, width), jnp.float32),
            pltpu.VMEM((hidden_units, width), jnp.float32),
            pltpu.VMEM((total, width), jnp.bfloat16),
            pltpu.VMEM((total, width), jnp.bfloat16),
            pltpu.VMEM((total, hidden_units), jnp.bfloat16),
            pltpu.VMEM((total, hidden_units), jnp.bfloat16),
            pltpu.SemaphoreType.DMA((len(args) - 1,)),
            pltpu.SemaphoreType.DMA((2, steps)),
        ],
        input_output_aliases={len(args) - 2: 0, len(args) - 1: 1} if have else {},
        compiler_params=pltpu.CompilerParams(vmem_limit_bytes=LIMIT),
        cost_estimate=pl.CostEstimate(
            flops=8 * total * width * hidden_units,
            transcendentals=0,
            bytes_accessed=4 * total * width,
        ),
        name="absorb",
    )(*args)


def adam_step(gradient, moment_one, moment_two):
    new_one = BETA_ONE * moment_one.astype(jnp.float32) + (1.0 - BETA_ONE) * gradient
    new_two = BETA_TWO * moment_two.astype(jnp.float32) + (1.0 - BETA_TWO) * gradient * gradient
    return new_one / (new_two * lax.rsqrt(new_two) + EPSILON)


def pick_copies(at, blocks, refs, targets, sems):
    starts, waits, refs = [], [], list(refs)
    for i, (test, _, second) in enumerate(blocks):
        first_ref = refs.pop(0)
        here = pltpu.make_async_copy(first_ref, targets[i], sems.at[i])
        waits.append(here)
        if second is None:
            starts.append(here.start)
            continue
        there = pltpu.make_async_copy(refs.pop(0), targets[i], sems.at[i])

        def start(here=here, there=there, test=test):
            pl.when(test(at))(here.start)
            pl.when(jnp.logical_not(test(at)))(there.start)

        starts.append(start)
    return starts, waits


def lay_rows(blocks_vmem, held, first_part):
    piece = blocks_vmem[0].shape[2]
    offset = 0
    for ref in blocks_vmem:
        count = ref.shape[1]
        for q in range(PIECES):
            held[offset : offset + count, q * piece : (q + 1) * piece] = ref[first_part + q]
        offset += count


def finish(place, half, my_index, leaving, tile_owner, blocks, w_up, w_down, sums, moments):
    arrays = flatten(blocks)
    width, hidden_units = w_up.shape
    tiles = tile_owner.shape[0]
    tile_rows = width // tiles
    total = sum(first.shape[1] for _, first, _ in blocks)
    step = width // PIECES
    each = tiles // PIECES
    count = len(blocks)
    rest = (w_up, w_down, sums[1], moments[2], moments[3], sums[0], moments[0], moments[1])

    def body(place_ref, half_ref, me, leave, owner, *refs):
        rows_in, refs = refs[: len(arrays)], refs[len(arrays) :]
        rest_in, refs = refs[: len(rest)], refs[len(rest) :]
        out_up, out_down, out_near, out_far = refs[:4]
        refs = refs[4:]
        rows_vmem, refs = refs[:count], refs[count:]
        rest_vmem, refs = refs[: len(rest)], refs[len(rest) :]
        up_ref, down_ref, old_down, md, vd, old_up, mu, vu = rest_vmem
        moved_up, moved_down, both, held_x, held_c, held_pre, held_hid = refs[:7]
        sems, up_sems, down_sems, tile_sems = refs[7:]
        starts, waits = pick_copies(place_ref[0], blocks, rows_in, rows_vmem, sems)
        others = [
            pltpu.make_async_copy(source, target, sems.at[count + i])
            for i, (source, target) in enumerate(zip(rest_in, rest_vmem))
        ]
        for start in starts:
            start()
        for copy in others:
            copy.start()
        keep = me[0] != leave[0]
        for copy in waits:
            copy.wait()
        lay_rows(rows_vmem, held_x, 0)
        lay_rows(rows_vmem, held_c, PIECES)
        for copy in others[:2]:
            copy.wait()
        row_terms(up_ref, down_ref, held_x, held_c, held_pre, held_hid, total)
        for copy in others[2:]:
            copy.wait()

        def leave_steps(j):
            span = pl.ds(pl.multiple_of(j * step, step), step)
            return (
                pltpu.make_async_copy(moved_up.at[span, :], out_up.at[span, :], up_sems.at[j]),
                pltpu.make_async_copy(moved_down.at[:, span], out_down.at[:, span], down_sems.at[j]),
            )

        def tile_copy(t, out):
            span = pl.ds(pl.multiple_of(t * tile_rows, tile_rows), tile_rows)
            return pltpu.make_async_copy(
                both.at[span, :], out.at[owner[t] >> 1], tile_sems.at[t]
            )

        def columns(j, carry):
            span = pl.ds(pl.multiple_of(j * step, step), step)
            grad = old_down[:, span] + column_sums(held_hid[...], held_c[:, span])
            step_down = adam_step(grad, md[:, span], vd[:, span])
            both[span, hidden_units:] = step_down.T.astype(jnp.bfloat16)
            moved_down[:, span] = jnp.where(keep, step_down, 0.0).astype(jnp.bfloat16)
            grad = old_up[:, span] + column_sums(held_pre[...], held_x[:, span])
            step_up = adam_step(grad.T, mu[span, :], vu[span, :])
            both[span, :hidden_units] = step_up.astype(jnp.bfloat16)
            moved_up[span, :] = jnp.where(keep, step_up, 0.0).astype(jnp.bfloat16)
            for k in range(each):
                t = j * each + k
                near = (owner[t] & 1) == half_ref[0]
                pl.when(near)(tile_copy(t, out_near).start)
                pl.when(jnp.logical_not(near))(tile_copy(t, out_far).start)
            for copy in leave_steps(j):
                copy.start()
            return carry

        def drain(j, carry):
            for copy in leave_steps(j):
                copy.wait()
            for k in range(each):
                tile_copy(j * each + k, out_near).wait()
            return carry

        lax.fori_loop(0, PIECES, columns, 0)
        lax.fori_loop(0, PIECES, drain, 0)

    tile_shape = jax.ShapeDtypeStruct((tiles // 2, tile_rows, 2 * hidden_units), jnp.bfloat16)
    return pl.pallas_call(
        body,
        out_shape=[
            jax.ShapeDtypeStruct((width, hidden_units), jnp.bfloat16),
            jax.ShapeDtypeStruct((hidden_units, width), jnp.bfloat16),
            tile_shape,
            tile_shape,
        ],
        in_specs=[SMEM] * 5 + [HBM] * (len(arrays) + len(rest)),
        out_specs=[HBM] * 4,
        scratch_shapes=[pltpu.VMEM(first.shape, first.dtype) for _, first, _ in blocks]
        + [pltpu.VMEM(a.shape, a.dtype) for a in rest]
        + [
            pltpu.VMEM((width, hidden_units), jnp.bfloat16),
            pltpu.VMEM((hidden_units, width), jnp.bfloat16),
            pltpu.VMEM((width, 2 * hidden_units), jnp.bfloat16),
            pltpu.VMEM((total, width), jnp.bfloat16),
            pltpu.VMEM((total, width), jnp.bfloat16),
            pltpu.VMEM((total, hidden_units), jnp.bfloat16),
            pltpu.VMEM((total, hidden_units), jnp.bfloat16),
            pltpu.SemaphoreType.DMA((count + len(rest),)),
            pltpu.SemaphoreType.DMA((PIECES,)),
            pltpu.SemaphoreType.DMA((PIECES,)),
            pltpu.SemaphoreType.DMA((tiles,)),
        ],
        compiler_params=pltpu.CompilerParams(vmem_limit_bytes=LIMIT),
        name="finish",
    )(place, half, my_index, leaving, tile_owner, *arrays, *rest)


def on_device(
    tokens, cotangent, gates, routes, w_up, w_down, m_up, v_up, m_down, v_down, leaving, tile_owner
):
    tok_count, width = tokens.shape
    piece = width // PIECES
    core = lax.axis_index("co")
    low = lax.axis_index("zl")
    half = lax.axis_index("zh")
    column = lax.axis_index(("y", "x"))
    place = jnp.where(core == 0, low, 3 - low)
    base = jnp.where(low <= 1, half, 1 - half)
    place_ref = place.reshape(1)

    outgoing = []
    for tag, group in zip(TAGS, SLOT_GROUPS):
        outgoing += prepare(
            base.reshape(1),
            tokens,
            cotangent,
            gates.reshape(1, tok_count),
            routes.reshape(1, tok_count),
            (group,),
        )

    def step(value, places):
        return lax.ppermute(value, ALL, stream_pairs(places))

    def swap(value):
        return lax.ppermute(value, ALL, swap_pairs())

    chunks = []
    previous = None
    for tag, (_, slots), sent in zip(TAGS, SLOT_GROUPS, outgoing):
        rows = sent.shape[0]
        if previous is not None:
            previous, sent = lax.optimization_barrier((previous, sent))
            chunks[-1][0] = previous
        previous = lax.all_to_all(
            sent.reshape(32, rows // 32, piece), ("co", "y", "x"), 0, 0, tiled=True
        ).reshape(rows, piece)
        chunks.append({"tag": tag, "slots": slots, 0: previous})

    def joined(first, second):
        return jnp.where(place == 3, first, second)

    for ch in chunks:
        tag = ch["tag"]
        ch[0] = arrange(ch[0], ch["slots"])
        ch[1] = step(ch[0], (0, 1, 2, 3))
        ch["s0"] = swap(ch[0])
        x2 = step(ch["s0"], (2,))
        y2 = step(ch[1], (0, 1, 3))
        ch["s1"] = swap(ch[1])
        x3 = step(ch[1], (2,))
        y3 = step(y2, (0, 1))
        ch[2] = joined(x2, y2)
        ch["s2"] = swap(ch[2])
        x4 = step(y2, (2,))
        y4 = step(y3, (1,))
        ch[3] = joined(x3, y3)
        ch["s3"] = swap(ch[3])
        ch[5] = step(y3, (2,))
        ch[4] = joined(x4, y4)
        ch["s4"] = swap(ch[4])
        ch[6] = step(y4, (2,))
        ch["s5"] = swap(ch[5])
        ch["s6"] = swap(ch[6])

    rules = {
        "o": (lambda at: at <= 1, 0, "s0"),
        "1": (lambda at: at < 3, 1, None),
        "p": (lambda at: at > 0, "s1", None),
        "2": (None, 2, None),
        "q": (None, "s2", None),
        "3": (None, 3, None),
        "r": (None, "s3", None),
        "4": (lambda at: at >= 2, 4, "s4"),
        "5": (lambda at: at == 3, 5, "s5"),
        "6": (lambda at: at == 3, 6, "s6"),
    }

    def blocks_of(words):
        blocks = []
        for word in words.split():
            ch = chunks[TAGS.index(word[0])]
            for letter in word[1:]:
                test, one, two = rules[letter]
                blocks.append((test, ch[one], None if two is None else ch[two]))
        return blocks

    sums = None
    for words in SUMS:
        sums = absorb(place_ref, blocks_of(words), w_up[0], w_down[0], sums)
    my_index = (column * 2 + half).reshape(1)
    leaver = leaving[0]

    update_up, update_down, near, far = finish(
        place_ref,
        half.reshape(1),
        my_index,
        leaving,
        tile_owner,
        blocks_of(LAST),
        w_up[0],
        w_down[0],
        sums,
        (m_up[0], v_up[0], m_down[0], v_down[0]),
    )

    def from_leaver(tiles):
        incoming = lax.all_to_all(tiles, ("y", "x"), 0, 0, tiled=True)
        return lax.dynamic_index_in_dim(incoming, leaver // 2, 0, keepdims=False)

    far, near = lax.optimization_barrier((far, near))
    far = from_leaver(far)
    crossed = lax.ppermute(far, ALL, across_pairs())
    near = from_leaver(near)
    mine = jnp.where(half == leaver % 2, near, crossed)[None]
    units = w_up.shape[2]
    return (update_up[None], update_down[None], mine[..., :units], mine[..., units:])


def solution(mesh):
    wide = Mesh(mesh.devices.reshape(4, 2, 4, 4, 2), ALL)
    dp = ("zl", "co")
    expert = ("y", "x", "zh")
    row = P(dp + expert, None)
    up = P(expert, None, dp)
    down = P(expert, dp, None)
    return jax.shard_map(
        on_device,
        mesh=wide,
        in_specs=(row, row, row, row, up, down, up, up, down, down, P(), P()),
        out_specs=(up, down, up, up),
        check_vma=False,
    )
```

```python
import jax
import jax.numpy as jnp
from jax import lax
from jax.experimental import pallas as pl
from jax.experimental.pallas import tpu as pltpu
from jax.sharding import Mesh
from jax.sharding import PartitionSpec as P


BETA_ONE = 0.9
BETA_TWO = 0.95
EPSILON = 1e-08

ALL = ("zl", "co", "y", "x", "zh")
SLOT_GROUPS = ((0, 2), (2, 3))
TAGS = ("a", "b")
UNSORTED = ("a",)
SUMS = ("ao1p2q3r", "a4 bo1p", "a56 b2q3r", "b45")
LAST = "b6"
PIECES = 4
VMEM = pl.BlockSpec(memory_space=pltpu.VMEM)
SMEM = pl.BlockSpec(memory_space=pltpu.SMEM)
HBM = pl.BlockSpec(memory_space=pltpu.MemorySpace.HBM)
LIMIT = 60 * 1024 * 1024


def device_id(z, core, y, x):
    return (((z % 4) * 2 + core) * 4 + y) * 8 + x * 2 + z // 4


def every():
    for z in range(8):
        for core in range(2):
            for y in range(4):
                for x in range(4):
                    yield z, core, y, x


def stream_pairs(places):
    pairs = []
    for z, core, y, x in every():
        place = z % 4 if core == 0 else 3 - z % 4
        if place in places:
            there = (z + (1 if core == 0 else -1)) % 8
            pairs.append((device_id(z, core, y, x), device_id(there, core, y, x)))
    return pairs


def swap_pairs():
    return [(device_id(z, c, y, x), device_id(z, 1 - c, y, x)) for z, c, y, x in every()]


def across_pairs():
    return [(device_id(z, c, y, x), device_id((z + 4) % 8, c, y, x)) for z, c, y, x in every()]


def over(value, divisor):
    if divisor & (divisor - 1) == 0:
        return value >> (divisor.bit_length() - 1)
    return (value * (-(-(1 << 18) // divisor))) >> 18


def prepare(base, tokens, cotangent, gates_row, routes_row, outs_slots):
    tok_count, width = tokens.shape
    piece = width // PIECES
    parts = 2 * PIECES

    def body(base_ref, x_ref, c_ref, g_ref, r_ref, *rest):
        outs, (held,) = rest[:-1], rest[-1:]
        routes = jnp.broadcast_to(r_ref[...], (tok_count, tok_count))
        routes_down = routes.T
        gate_down = jnp.broadcast_to(g_ref[...], (tok_count, tok_count)).T
        at_row = lax.broadcasted_iota(jnp.int32, (tok_count, tok_count), 0)
        at_col = lax.broadcasted_iota(jnp.int32, (tok_count, tok_count), 1)
        before = jnp.where((routes_down == routes) & (at_row < at_col), 1, 0)
        rank = jnp.sum(before, axis=0, keepdims=True)
        code = r_ref[...] * 8 + rank
        for q in range(PIECES):
            held[q * tok_count : (q + 1) * tok_count, :] = x_ref[:, q * piece : (q + 1) * piece]
            for j in range(piece // 128):
                cols = c_ref[:, q * piece + j * 128 : q * piece + (j + 1) * 128]
                held[
                    (PIECES + q) * tok_count : (PIECES + q + 1) * tok_count,
                    j * 128 : (j + 1) * 128,
                ] = (gate_down * cols.astype(jnp.float32)).astype(jnp.bfloat16)
        for out, (first, slots) in zip(outs, outs_slots):
            rows = 32 * parts * slots
            row = lax.broadcasted_iota(jnp.int32, (rows, tok_count), 0)
            group = over(row, slots)
            slot = row - group * slots
            part = group & (parts - 1)
            dest = group >> 3
            expert = ((dest & 15) << 1) | (base_ref[0] ^ (dest >> 4))
            hit = (expert * 8 + (slot + first)) == code
            picker = jnp.concatenate(
                [
                    jnp.where(hit & (part == q), 1.0, 0.0).astype(jnp.bfloat16)
                    for q in range(parts)
                ],
                axis=1,
            )
            out[...] = jnp.dot(
                picker, held[...], preferred_element_type=jnp.float32
            ).astype(jnp.bfloat16)

    return pl.pallas_call(
        body,
        out_shape=[
            jax.ShapeDtypeStruct((32 * parts * slots, piece), jnp.bfloat16)
            for _, slots in outs_slots
        ],
        in_specs=[SMEM, VMEM, VMEM, VMEM, VMEM],
        out_specs=[VMEM] * len(outs_slots),
        scratch_shapes=[pltpu.VMEM((parts * tok_count, piece), jnp.bfloat16)],
        compiler_params=pltpu.CompilerParams(vmem_limit_bytes=LIMIT),
        name="prepare",
    )(base, tokens, cotangent, gates_row, routes_row)


def sorter(slots):
    rows = 16 * 8 * slots
    row = lax.broadcasted_iota(jnp.int32, (rows, rows), 0)
    col = lax.broadcasted_iota(jnp.int32, (rows, rows), 1)
    part = over(row, 16 * slots)
    rest = row - part * (16 * slots)
    sender = over(rest, slots)
    slot = rest - sender * slots
    return jnp.where(col == sender * (8 * slots) + part * slots + slot, 1.0, 0.0).astype(
        jnp.bfloat16
    )


def arrange(received, slots):
    _, piece = received.shape
    count = 16 * slots

    def body(in_ref, out_ref):
        order = sorter(slots)
        for half in range(2):
            block = in_ref[half * 8 * count : (half + 1) * 8 * count, :]
            ordered = jnp.dot(order, block, preferred_element_type=jnp.float32)
            ordered = ordered.astype(jnp.bfloat16)
            for q in range(2 * PIECES):
                out_ref[q, half * count : (half + 1) * count, :] = ordered[
                    q * count : (q + 1) * count, :
                ]

    return pl.pallas_call(
        body,
        out_shape=jax.ShapeDtypeStruct((2 * PIECES, 2 * count, piece), jnp.bfloat16),
        in_specs=[VMEM],
        out_specs=VMEM,
        compiler_params=pltpu.CompilerParams(vmem_limit_bytes=LIMIT),
        name="arrange",
    )(received)


def flatten(blocks):
    arrays = []
    for _, first, second in blocks:
        arrays.append(first)
        if second is not None:
            arrays.append(second)
    return arrays


def rows_in(block):
    return block.shape[1] if len(block.shape) == 3 else block.shape[0] // (2 * PIECES)


def gather_rows(at, blocks, refs, held_x, held_c):
    refs = list(refs)
    piece = refs[0].shape[-1]
    offset = 0
    orders = {}
    for test, first, second in blocks:
        first_ref = refs.pop(0)
        second_ref = refs.pop(0) if second is not None else None
        count = rows_in(first)
        if len(first.shape) == 3:
            for q in range(2 * PIECES):
                part = first_ref[q]
                if second_ref is not None:
                    part = jnp.where(test(at), part, second_ref[q])
                elif test is not None and q >= PIECES:
                    part = jnp.where(test(at), part, jnp.zeros_like(part))
                held = held_x if q < PIECES else held_c
                left = (q % PIECES) * piece
                held[offset : offset + count, left : left + piece] = part
        else:
            slots = count // 32
            if slots not in orders:
                orders[slots] = sorter(slots)
            order = orders[slots]
            rows, some = 8 * count // 2, count // 2

            def sort_half(
                half,
                carry,
                first_ref=first_ref,
                second_ref=second_ref,
                order=order,
                test=test,
                offset=offset,
                rows=rows,
                some=some,
            ):
                span = pl.ds(pl.multiple_of(half * rows, rows), rows)
                block = first_ref[span, :]
                if second_ref is not None:
                    block = jnp.where(test(at), block, second_ref[span, :])
                ordered = jnp.dot(order, block, preferred_element_type=jnp.float32)
                target = pl.ds(pl.multiple_of(offset + half * some, 16), some)
                for q in range(2 * PIECES):
                    part = ordered[q * some : (q + 1) * some, :]
                    if second_ref is None and test is not None and q >= PIECES:
                        part = jnp.where(test(at), part, 0.0)
                    held = held_x if q < PIECES else held_c
                    left = (q % PIECES) * piece
                    held[target, left : left + piece] = part.astype(jnp.bfloat16)
                return carry

            lax.fori_loop(0, 2, sort_half, 0)
        offset += count


def row_terms(up_ref, down_ref, held_x, held_c, held_pre, held_hid, tile):
    def rows_of(i, carry):
        span = pl.ds(pl.multiple_of(i * tile, tile), tile)
        preact = jnp.dot(held_x[span, :], up_ref[...], preferred_element_type=jnp.float32)
        back_grad = lax.dot_general(
            held_c[span, :],
            down_ref[...],
            (((1,), (1,)), ((), ())),
            preferred_element_type=jnp.float32,
        )
        squash = jax.nn.sigmoid(preact)
        held_hid[span, :] = (preact * squash).astype(jnp.bfloat16)
        slope = squash * (1.0 + preact * (1.0 - squash))
        held_pre[span, :] = (back_grad * slope).astype(jnp.bfloat16)
        return carry

    lax.fori_loop(0, held_x.shape[0] // tile, rows_of, 0)


def column_sums(left, right):
    return lax.dot_general(left, right, (((0,), (0,)), ((), ())), preferred_element_type=jnp.float32)


def absorb(place, blocks, w_up, w_down, sums):
    arrays = flatten(blocks)
    width, hidden_units = w_up.shape
    total = sum(rows_in(first) for _, first, _ in blocks)
    have = sums is not None
    steps = 7
    step = width // steps
    tile = total // 2 if total > 128 else total
    count = len(arrays)

    def body(place_ref, *refs):
        hbm_in, refs = refs[: count + 2], refs[count + 2 :]
        if have:
            hbm_in, refs = hbm_in + refs[:2], refs[2:]
        outs, refs = refs[:2], refs[2:]
        vmem_in, refs = list(refs[: count + 2]), refs[count + 2 :]
        acc_up, acc_down, held_x, held_c, held_pre, held_hid, in_sems, out_sems = refs
        if have:
            vmem_in += [acc_up, acc_down]
        copies = [
            pltpu.make_async_copy(source, target, in_sems.at[i])
            for i, (source, target) in enumerate(zip(hbm_in, vmem_in))
        ]
        for copy in copies:
            copy.start()
        for copy in copies[:count]:
            copy.wait()
        gather_rows(place_ref[0], blocks, vmem_in[:count], held_x, held_c)
        for copy in copies[count : count + 2]:
            copy.wait()
        row_terms(vmem_in[count], vmem_in[count + 1], held_x, held_c, held_pre, held_hid, tile)
        for copy in copies[count + 2 :]:
            copy.wait()

        def leave(j):
            span = pl.ds(pl.multiple_of(j * step, step), step)
            return [
                pltpu.make_async_copy(acc.at[:, span], out.at[:, span], out_sems.at[k, j])
                for k, (acc, out) in enumerate(zip((acc_up, acc_down), outs))
            ]

        def columns(j, carry):
            span = pl.ds(pl.multiple_of(j * step, step), step)
            part_up = column_sums(held_pre[...], held_x[:, span])
            acc_up[:, span] = part_up + acc_up[:, span] if have else part_up
            part_down = column_sums(held_hid[...], held_c[:, span])
            acc_down[:, span] = part_down + acc_down[:, span] if have else part_down
            for copy in leave(j):
                copy.start()
            return carry

        def drain(j, carry):
            for copy in leave(j):
                copy.wait()
            return carry

        lax.fori_loop(0, steps, columns, 0)
        lax.fori_loop(0, steps, drain, 0)

    shape = jax.ShapeDtypeStruct((hidden_units, width), jnp.float32)
    args = [place, *arrays, w_up, w_down] + (list(sums) if have else [])
    return pl.pallas_call(
        body,
        out_shape=[shape, shape],
        in_specs=[SMEM] + [HBM] * (len(args) - 1),
        out_specs=[HBM, HBM],
        scratch_shapes=[pltpu.VMEM(a.shape, a.dtype) for a in (*arrays, w_up, w_down)]
        + [
            pltpu.VMEM((hidden_units, width), jnp.float32),
            pltpu.VMEM((hidden_units, width), jnp.float32),
            pltpu.VMEM((total, width), jnp.bfloat16),
            pltpu.VMEM((total, width), jnp.bfloat16),
            pltpu.VMEM((total, hidden_units), jnp.bfloat16),
            pltpu.VMEM((total, hidden_units), jnp.bfloat16),
            pltpu.SemaphoreType.DMA((len(args) - 1,)),
            pltpu.SemaphoreType.DMA((2, steps)),
        ],
        input_output_aliases={len(args) - 2: 0, len(args) - 1: 1} if have else {},
        compiler_params=pltpu.CompilerParams(vmem_limit_bytes=LIMIT),
        cost_estimate=pl.CostEstimate(
            flops=8 * total * width * hidden_units,
            transcendentals=0,
            bytes_accessed=4 * total * width,
        ),
        name="absorb",
    )(*args)


def adam_step(gradient, moment_one, moment_two):
    new_one = BETA_ONE * moment_one.astype(jnp.float32) + (1.0 - BETA_ONE) * gradient
    new_two = BETA_TWO * moment_two.astype(jnp.float32) + (1.0 - BETA_TWO) * gradient * gradient
    return new_one / (new_two * lax.rsqrt(new_two) + EPSILON)


def pick_copies(at, blocks, refs, targets, sems):
    starts, waits, refs = [], [], list(refs)
    for i, (test, _, second) in enumerate(blocks):
        first_ref = refs.pop(0)
        here = pltpu.make_async_copy(first_ref, targets[i], sems.at[i])
        waits.append(here)
        if second is None:
            starts.append(here.start)
            continue
        there = pltpu.make_async_copy(refs.pop(0), targets[i], sems.at[i])

        def start(here=here, there=there, test=test):
            pl.when(test(at))(here.start)
            pl.when(jnp.logical_not(test(at)))(there.start)

        starts.append(start)
    return starts, waits


def lay_rows(blocks_vmem, held, first_part):
    piece = blocks_vmem[0].shape[2]
    offset = 0
    for ref in blocks_vmem:
        count = ref.shape[1]
        for q in range(PIECES):
            held[offset : offset + count, q * piece : (q + 1) * piece] = ref[first_part + q]
        offset += count


def finish(place, half, my_index, leaving, tile_owner, blocks, w_up, w_down, sums, moments):
    arrays = flatten(blocks)
    width, hidden_units = w_up.shape
    tiles = tile_owner.shape[0]
    tile_rows = width // tiles
    total = sum(first.shape[1] for _, first, _ in blocks)
    step = width // PIECES
    each = tiles // PIECES
    count = len(blocks)
    rest = (w_up, w_down, sums[1], moments[2], moments[3], sums[0], moments[0], moments[1])

    def body(place_ref, half_ref, me, leave, owner, *refs):
        block_refs, refs = refs[: len(arrays)], refs[len(arrays) :]
        rest_in, refs = refs[: len(rest)], refs[len(rest) :]
        out_up, out_down, out_near, out_far = refs[:4]
        refs = refs[4:]
        rows_vmem, refs = refs[:count], refs[count:]
        rest_vmem, refs = refs[: len(rest)], refs[len(rest) :]
        up_ref, down_ref, old_down, md, vd, old_up, mu, vu = rest_vmem
        moved_up, moved_down, both, held_x, held_c, held_pre, held_hid = refs[:7]
        sems, up_sems, down_sems, tile_sems = refs[7:]
        starts, waits = pick_copies(place_ref[0], blocks, block_refs, rows_vmem, sems)
        others = [
            pltpu.make_async_copy(source, target, sems.at[count + i])
            for i, (source, target) in enumerate(zip(rest_in, rest_vmem))
        ]
        for start in starts:
            start()
        for copy in others:
            copy.start()
        keep = me[0] != leave[0]
        for copy in waits:
            copy.wait()
        lay_rows(rows_vmem, held_x, 0)
        lay_rows(rows_vmem, held_c, PIECES)
        for copy in others[:2]:
            copy.wait()
        row_terms(up_ref, down_ref, held_x, held_c, held_pre, held_hid, total)
        for copy in others[2:]:
            copy.wait()

        def leave_steps(j):
            span = pl.ds(pl.multiple_of(j * step, step), step)
            return (
                pltpu.make_async_copy(moved_up.at[span, :], out_up.at[span, :], up_sems.at[j]),
                pltpu.make_async_copy(moved_down.at[:, span], out_down.at[:, span], down_sems.at[j]),
            )

        def tile_copy(t, out):
            span = pl.ds(pl.multiple_of(t * tile_rows, tile_rows), tile_rows)
            return pltpu.make_async_copy(
                both.at[span, :], out.at[owner[t] >> 1], tile_sems.at[t]
            )

        def columns(j, carry):
            span = pl.ds(pl.multiple_of(j * step, step), step)
            grad = old_down[:, span] + column_sums(held_hid[...], held_c[:, span])
            step_down = adam_step(grad, md[:, span], vd[:, span])
            both[span, hidden_units:] = step_down.T.astype(jnp.bfloat16)
            moved_down[:, span] = jnp.where(keep, step_down, 0.0).astype(jnp.bfloat16)
            grad = old_up[:, span] + column_sums(held_pre[...], held_x[:, span])
            step_up = adam_step(grad.T, mu[span, :], vu[span, :])
            both[span, :hidden_units] = step_up.astype(jnp.bfloat16)
            moved_up[span, :] = jnp.where(keep, step_up, 0.0).astype(jnp.bfloat16)
            for k in range(each):
                t = j * each + k
                near = (owner[t] & 1) == half_ref[0]
                pl.when(near)(tile_copy(t, out_near).start)
                pl.when(jnp.logical_not(near))(tile_copy(t, out_far).start)
            for copy in leave_steps(j):
                copy.start()
            return carry

        def drain(j, carry):
            for copy in leave_steps(j):
                copy.wait()
            for k in range(each):
                tile_copy(j * each + k, out_near).wait()
            return carry

        lax.fori_loop(0, PIECES, columns, 0)
        lax.fori_loop(0, PIECES, drain, 0)

    tile_shape = jax.ShapeDtypeStruct((tiles // 2, tile_rows, 2 * hidden_units), jnp.bfloat16)
    return pl.pallas_call(
        body,
        out_shape=[
            jax.ShapeDtypeStruct((width, hidden_units), jnp.bfloat16),
            jax.ShapeDtypeStruct((hidden_units, width), jnp.bfloat16),
            tile_shape,
            tile_shape,
        ],
        in_specs=[SMEM] * 5 + [HBM] * (len(arrays) + len(rest)),
        out_specs=[HBM] * 4,
        scratch_shapes=[pltpu.VMEM(first.shape, first.dtype) for _, first, _ in blocks]
        + [pltpu.VMEM(a.shape, a.dtype) for a in rest]
        + [
            pltpu.VMEM((width, hidden_units), jnp.bfloat16),
            pltpu.VMEM((hidden_units, width), jnp.bfloat16),
            pltpu.VMEM((width, 2 * hidden_units), jnp.bfloat16),
            pltpu.VMEM((total, width), jnp.bfloat16),
            pltpu.VMEM((total, width), jnp.bfloat16),
            pltpu.VMEM((total, hidden_units), jnp.bfloat16),
            pltpu.VMEM((total, hidden_units), jnp.bfloat16),
            pltpu.SemaphoreType.DMA((count + len(rest),)),
            pltpu.SemaphoreType.DMA((PIECES,)),
            pltpu.SemaphoreType.DMA((PIECES,)),
            pltpu.SemaphoreType.DMA((tiles,)),
        ],
        compiler_params=pltpu.CompilerParams(vmem_limit_bytes=LIMIT),
        name="finish",
    )(place, half, my_index, leaving, tile_owner, *arrays, *rest)


def on_device(
    tokens, cotangent, gates, routes, w_up, w_down, m_up, v_up, m_down, v_down, leaving, tile_owner
):
    tok_count, width = tokens.shape
    piece = width // PIECES
    core = lax.axis_index("co")
    low = lax.axis_index("zl")
    half = lax.axis_index("zh")
    column = lax.axis_index(("y", "x"))
    place = jnp.where(core == 0, low, 3 - low)
    base = jnp.where(low <= 1, half, 1 - half)
    place_ref = place.reshape(1)

    outgoing = []
    for tag, group in zip(TAGS, SLOT_GROUPS):
        outgoing += prepare(
            base.reshape(1),
            tokens,
            cotangent,
            gates.reshape(1, tok_count),
            routes.reshape(1, tok_count),
            (group,),
        )

    def step(value, places):
        return lax.ppermute(value, ALL, stream_pairs(places))

    def swap(value):
        return lax.ppermute(value, ALL, swap_pairs())

    chunks = []
    previous = None
    for tag, (_, slots), sent in zip(TAGS, SLOT_GROUPS, outgoing):
        rows = sent.shape[0]
        if previous is not None:
            previous, sent = lax.optimization_barrier((previous, sent))
            chunks[-1][0] = previous
        previous = lax.all_to_all(
            sent.reshape(32, rows // 32, piece), ("co", "y", "x"), 0, 0, tiled=True
        ).reshape(rows, piece)
        chunks.append({"tag": tag, "slots": slots, 0: previous})

    def joined(first, second):
        return jnp.where(place == 3, first, second)

    for ch in chunks:
        tag = ch["tag"]
        if tag not in UNSORTED:
            ch[0] = arrange(ch[0], ch["slots"])
        ch[1] = step(ch[0], (0, 1, 2, 3))
        ch["s0"] = swap(ch[0])
        x2 = step(ch["s0"], (2,))
        y2 = step(ch[1], (0, 1, 3))
        ch["s1"] = swap(ch[1])
        x3 = step(ch[1], (2,))
        y3 = step(y2, (0, 1))
        ch[2] = joined(x2, y2)
        ch["s2"] = swap(ch[2])
        x4 = step(y2, (2,))
        y4 = step(y3, (1,))
        ch[3] = joined(x3, y3)
        ch["s3"] = swap(ch[3])
        ch[5] = step(y3, (2,))
        ch[4] = joined(x4, y4)
        ch["s4"] = swap(ch[4])
        ch[6] = step(y4, (2,))
        ch["s5"] = swap(ch[5])
        ch["s6"] = swap(ch[6])

    rules = {
        "o": (lambda at: at <= 1, 0, "s0"),
        "1": (lambda at: at < 3, 1, None),
        "p": (lambda at: at > 0, "s1", None),
        "2": (None, 2, None),
        "q": (None, "s2", None),
        "3": (None, 3, None),
        "r": (None, "s3", None),
        "4": (lambda at: at >= 2, 4, "s4"),
        "5": (lambda at: at == 3, 5, "s5"),
        "6": (lambda at: at == 3, 6, "s6"),
    }

    def blocks_of(words):
        blocks = []
        for word in words.split():
            ch = chunks[TAGS.index(word[0])]
            for letter in word[1:]:
                test, one, two = rules[letter]
                blocks.append((test, ch[one], None if two is None else ch[two]))
        return blocks

    sums = None
    for words in SUMS:
        sums = absorb(place_ref, blocks_of(words), w_up[0], w_down[0], sums)
    my_index = (column * 2 + half).reshape(1)
    leaver = leaving[0]

    update_up, update_down, near, far = finish(
        place_ref,
        half.reshape(1),
        my_index,
        leaving,
        tile_owner,
        blocks_of(LAST),
        w_up[0],
        w_down[0],
        sums,
        (m_up[0], v_up[0], m_down[0], v_down[0]),
    )

    def from_leaver(tiles):
        incoming = lax.all_to_all(tiles, ("y", "x"), 0, 0, tiled=True)
        return lax.dynamic_index_in_dim(incoming, leaver // 2, 0, keepdims=False)

    far, near = lax.optimization_barrier((far, near))
    far = from_leaver(far)
    crossed = lax.ppermute(far, ALL, across_pairs())
    near = from_leaver(near)
    mine = jnp.where(half == leaver % 2, near, crossed)[None]
    units = w_up.shape[2]
    return (update_up[None], update_down[None], mine[..., :units], mine[..., units:])


def solution(mesh):
    wide = Mesh(mesh.devices.reshape(4, 2, 4, 4, 2), ALL)
    dp = ("zl", "co")
    expert = ("y", "x", "zh")
    row = P(dp + expert, None)
    up = P(expert, None, dp)
    down = P(expert, dp, None)
    return jax.shard_map(
        on_device,
        mesh=wide,
        in_specs=(row, row, row, row, up, down, up, up, down, down, P(), P()),
        out_specs=(up, down, up, up),
        check_vma=False,
    )
```

```python
import jax
import jax.numpy as jnp
from jax import lax
from jax.experimental import pallas as pl
from jax.experimental.pallas import tpu as pltpu
from jax.sharding import Mesh
from jax.sharding import PartitionSpec as P


BETA_ONE = 0.9
BETA_TWO = 0.95
EPSILON = 1e-08

ALL = ("zl", "co", "y", "x", "zh")
SLOT_GROUPS = ((0, 2), (2, 3))
TAGS = ("a", "b")
UNSORTED = ("a",)
SUMS = ("ao1p2q3r", "a4 bo1p", "a56 b2q3r", "b45")
LAST = "b6"
PIECES = 4
VMEM = pl.BlockSpec(memory_space=pltpu.VMEM)
SMEM = pl.BlockSpec(memory_space=pltpu.SMEM)
HBM = pl.BlockSpec(memory_space=pltpu.MemorySpace.HBM)
LIMIT = 60 * 1024 * 1024


def device_id(z, core, y, x):
    return (((z % 4) * 2 + core) * 4 + y) * 8 + x * 2 + z // 4


def every():
    for z in range(8):
        for core in range(2):
            for y in range(4):
                for x in range(4):
                    yield z, core, y, x


def stream_pairs(places):
    pairs = []
    for z, core, y, x in every():
        place = z % 4 if core == 0 else 3 - z % 4
        if place in places:
            there = (z + (1 if core == 0 else -1)) % 8
            pairs.append((device_id(z, core, y, x), device_id(there, core, y, x)))
    return pairs


def swap_pairs():
    return [(device_id(z, c, y, x), device_id(z, 1 - c, y, x)) for z, c, y, x in every()]


def across_pairs():
    return [(device_id(z, c, y, x), device_id((z + 4) % 8, c, y, x)) for z, c, y, x in every()]


def over(value, divisor):
    if divisor & (divisor - 1) == 0:
        return value >> (divisor.bit_length() - 1)
    return (value * (-(-(1 << 18) // divisor))) >> 18


def prepare(base, tokens, cotangent, gates_row, routes_row, outs_slots):
    tok_count, width = tokens.shape
    piece = width // PIECES
    parts = 2 * PIECES

    def body(base_ref, x_ref, c_ref, g_ref, r_ref, *rest):
        outs, (held,) = rest[:-1], rest[-1:]
        routes = jnp.broadcast_to(r_ref[...], (tok_count, tok_count))
        routes_down = routes.T
        gate_down = jnp.broadcast_to(g_ref[...], (tok_count, tok_count)).T
        at_row = lax.broadcasted_iota(jnp.int32, (tok_count, tok_count), 0)
        at_col = lax.broadcasted_iota(jnp.int32, (tok_count, tok_count), 1)
        before = jnp.where((routes_down == routes) & (at_row < at_col), 1, 0)
        rank = jnp.sum(before, axis=0, keepdims=True)
        code = r_ref[...] * 8 + rank
        for q in range(PIECES):
            held[q * tok_count : (q + 1) * tok_count, :] = x_ref[:, q * piece : (q + 1) * piece]
            for j in range(piece // 128):
                cols = c_ref[:, q * piece + j * 128 : q * piece + (j + 1) * 128]
                held[
                    (PIECES + q) * tok_count : (PIECES + q + 1) * tok_count,
                    j * 128 : (j + 1) * 128,
                ] = (gate_down * cols.astype(jnp.float32)).astype(jnp.bfloat16)
        for out, (first, slots) in zip(outs, outs_slots):
            rows = 32 * parts * slots
            row = lax.broadcasted_iota(jnp.int32, (rows, tok_count), 0)
            group = over(row, slots)
            slot = row - group * slots
            part = group & (parts - 1)
            dest = group >> 3
            expert = ((dest & 15) << 1) | (base_ref[0] ^ (dest >> 4))
            hit = (expert * 8 + (slot + first)) == code
            picker = jnp.concatenate(
                [
                    jnp.where(hit & (part == q), 1.0, 0.0).astype(jnp.bfloat16)
                    for q in range(parts)
                ],
                axis=1,
            )
            out[...] = jnp.dot(
                picker, held[...], preferred_element_type=jnp.float32
            ).astype(jnp.bfloat16)

    return pl.pallas_call(
        body,
        out_shape=[
            jax.ShapeDtypeStruct((32 * parts * slots, piece), jnp.bfloat16)
            for _, slots in outs_slots
        ],
        in_specs=[SMEM, VMEM, VMEM, VMEM, VMEM],
        out_specs=[VMEM] * len(outs_slots),
        scratch_shapes=[pltpu.VMEM((parts * tok_count, piece), jnp.bfloat16)],
        compiler_params=pltpu.CompilerParams(vmem_limit_bytes=LIMIT),
        name="prepare",
    )(base, tokens, cotangent, gates_row, routes_row)


def sorter(slots):
    rows = 16 * 8 * slots
    row = lax.broadcasted_iota(jnp.int32, (rows, rows), 0)
    col = lax.broadcasted_iota(jnp.int32, (rows, rows), 1)
    part = over(row, 16 * slots)
    rest = row - part * (16 * slots)
    sender = over(rest, slots)
    slot = rest - sender * slots
    return jnp.where(col == sender * (8 * slots) + part * slots + slot, 1.0, 0.0).astype(
        jnp.bfloat16
    )


def arrange(received, slots):
    _, piece = received.shape
    count = 16 * slots

    def body(in_ref, out_ref):
        order = sorter(slots)
        for half in range(2):
            block = in_ref[half * 8 * count : (half + 1) * 8 * count, :]
            ordered = jnp.dot(order, block, preferred_element_type=jnp.float32)
            ordered = ordered.astype(jnp.bfloat16)
            for q in range(2 * PIECES):
                out_ref[q, half * count : (half + 1) * count, :] = ordered[
                    q * count : (q + 1) * count, :
                ]

    return pl.pallas_call(
        body,
        out_shape=jax.ShapeDtypeStruct((2 * PIECES, 2 * count, piece), jnp.bfloat16),
        in_specs=[VMEM],
        out_specs=VMEM,
        compiler_params=pltpu.CompilerParams(vmem_limit_bytes=LIMIT),
        name="arrange",
    )(received)


def flatten(blocks):
    arrays = []
    for _, first, second in blocks:
        arrays.append(first)
        if second is not None:
            arrays.append(second)
    return arrays


def rows_in(block):
    return block.shape[1] if len(block.shape) == 3 else block.shape[0] // (2 * PIECES)


def gather_rows(at, blocks, refs, held_x, held_c):
    refs = list(refs)
    piece = refs[0].shape[-1]
    offset = 0
    orders = {}
    for test, first, second in blocks:
        first_ref = refs.pop(0)
        second_ref = refs.pop(0) if second is not None else None
        count = rows_in(first)
        if len(first.shape) == 3:
            for q in range(2 * PIECES):
                part = first_ref[q]
                if second_ref is not None:
                    part = jnp.where(test(at), part, second_ref[q])
                elif test is not None and q >= PIECES:
                    part = jnp.where(test(at), part, jnp.zeros_like(part))
                held = held_x if q < PIECES else held_c
                left = (q % PIECES) * piece
                held[offset : offset + count, left : left + piece] = part
        else:
            slots = count // 32
            if slots not in orders:
                orders[slots] = sorter(slots)
            order = orders[slots]
            rows, some = 8 * count // 2, count // 2

            def sort_half(
                half,
                carry,
                first_ref=first_ref,
                second_ref=second_ref,
                order=order,
                test=test,
                offset=offset,
                rows=rows,
                some=some,
            ):
                span = pl.ds(pl.multiple_of(half * rows, rows), rows)
                block = first_ref[span, :]
                if second_ref is not None:
                    block = jnp.where(test(at), block, second_ref[span, :])
                ordered = jnp.dot(order, block, preferred_element_type=jnp.float32)
                target = pl.ds(pl.multiple_of(offset + half * some, 16), some)
                for q in range(2 * PIECES):
                    part = ordered[q * some : (q + 1) * some, :]
                    if second_ref is None and test is not None and q >= PIECES:
                        part = jnp.where(test(at), part, 0.0)
                    held = held_x if q < PIECES else held_c
                    left = (q % PIECES) * piece
                    held[target, left : left + piece] = part.astype(jnp.bfloat16)
                return carry

            lax.fori_loop(0, 2, sort_half, 0)
        offset += count


def row_terms(up_ref, down_ref, held_x, held_c, held_pre, held_hid, tile):
    def rows_of(i, carry):
        span = pl.ds(pl.multiple_of(i * tile, tile), tile)
        preact = jnp.dot(held_x[span, :], up_ref[...], preferred_element_type=jnp.float32)
        back_grad = lax.dot_general(
            held_c[span, :],
            down_ref[...],
            (((1,), (1,)), ((), ())),
            preferred_element_type=jnp.float32,
        )
        squash = jax.nn.sigmoid(preact)
        held_hid[span, :] = (preact * squash).astype(jnp.bfloat16)
        slope = squash * (1.0 + preact * (1.0 - squash))
        held_pre[span, :] = (back_grad * slope).astype(jnp.bfloat16)
        return carry

    lax.fori_loop(0, held_x.shape[0] // tile, rows_of, 0)


def column_sums(left, right):
    return lax.dot_general(left, right, (((0,), (0,)), ((), ())), preferred_element_type=jnp.float32)


def absorb(place, blocks, w_up, w_down, sums):
    arrays = flatten(blocks)
    width, hidden_units = w_up.shape
    total = sum(rows_in(first) for _, first, _ in blocks)
    have = sums is not None
    steps = 7
    step = width // steps
    tile = total // 2 if total > 128 else total
    count = len(arrays)

    def body(place_ref, *refs):
        hbm_in, refs = refs[: count + 2], refs[count + 2 :]
        if have:
            hbm_in, refs = hbm_in + refs[:2], refs[2:]
        outs, refs = refs[:2], refs[2:]
        vmem_in, refs = list(refs[: count + 2]), refs[count + 2 :]
        acc_up, acc_down, held_x, held_c, held_pre, held_hid, in_sems, out_sems = refs
        if have:
            vmem_in += [acc_up, acc_down]
        copies = [
            pltpu.make_async_copy(source, target, in_sems.at[i])
            for i, (source, target) in enumerate(zip(hbm_in, vmem_in))
        ]
        for copy in copies:
            copy.start()
        for copy in copies[:count]:
            copy.wait()
        gather_rows(place_ref[0], blocks, vmem_in[:count], held_x, held_c)
        for copy in copies[count : count + 2]:
            copy.wait()
        row_terms(vmem_in[count], vmem_in[count + 1], held_x, held_c, held_pre, held_hid, tile)
        for copy in copies[count + 2 :]:
            copy.wait()

        def leave(j):
            span = pl.ds(pl.multiple_of(j * step, step), step)
            return [
                pltpu.make_async_copy(acc.at[:, span], out.at[:, span], out_sems.at[k, j])
                for k, (acc, out) in enumerate(zip((acc_up, acc_down), outs))
            ]

        def columns(j, carry):
            span = pl.ds(pl.multiple_of(j * step, step), step)
            part_up = column_sums(held_pre[...], held_x[:, span])
            acc_up[:, span] = part_up + acc_up[:, span] if have else part_up
            part_down = column_sums(held_hid[...], held_c[:, span])
            acc_down[:, span] = part_down + acc_down[:, span] if have else part_down
            for copy in leave(j):
                copy.start()
            return carry

        def drain(j, carry):
            for copy in leave(j):
                copy.wait()
            return carry

        lax.fori_loop(0, steps, columns, 0)
        lax.fori_loop(0, steps, drain, 0)

    shape = jax.ShapeDtypeStruct((hidden_units, width), jnp.float32)
    args = [place, *arrays, w_up, w_down] + (list(sums) if have else [])
    return pl.pallas_call(
        body,
        out_shape=[shape, shape],
        in_specs=[SMEM] + [HBM] * (len(args) - 1),
        out_specs=[HBM, HBM],
        scratch_shapes=[pltpu.VMEM(a.shape, a.dtype) for a in (*arrays, w_up, w_down)]
        + [
            pltpu.VMEM((hidden_units, width), jnp.float32),
            pltpu.VMEM((hidden_units, width), jnp.float32),
            pltpu.VMEM((total, width), jnp.bfloat16),
            pltpu.VMEM((total, width), jnp.bfloat16),
            pltpu.VMEM((total, hidden_units), jnp.bfloat16),
            pltpu.VMEM((total, hidden_units), jnp.bfloat16),
            pltpu.SemaphoreType.DMA((len(args) - 1,)),
            pltpu.SemaphoreType.DMA((2, steps)),
        ],
        input_output_aliases={len(args) - 2: 0, len(args) - 1: 1} if have else {},
        compiler_params=pltpu.CompilerParams(vmem_limit_bytes=LIMIT),
        cost_estimate=pl.CostEstimate(
            flops=8 * total * width * hidden_units,
            transcendentals=0,
            bytes_accessed=4 * total * width,
        ),
        name="absorb",
    )(*args)


def adam_step(gradient, moment_one, moment_two):
    new_one = BETA_ONE * moment_one.astype(jnp.float32) + (1.0 - BETA_ONE) * gradient
    new_two = BETA_TWO * moment_two.astype(jnp.float32) + (1.0 - BETA_TWO) * gradient * gradient
    return new_one / (new_two * lax.rsqrt(new_two) + EPSILON)


def pick_copies(at, blocks, refs, targets, sems):
    starts, waits, refs = [], [], list(refs)
    for i, (test, _, second) in enumerate(blocks):
        first_ref = refs.pop(0)
        here = pltpu.make_async_copy(first_ref, targets[i], sems.at[i])
        waits.append(here)
        if second is None:
            starts.append(here.start)
            continue
        there = pltpu.make_async_copy(refs.pop(0), targets[i], sems.at[i])

        def start(here=here, there=there, test=test):
            pl.when(test(at))(here.start)
            pl.when(jnp.logical_not(test(at)))(there.start)

        starts.append(start)
    return starts, waits


def lay_rows(blocks_vmem, held, first_part):
    piece = blocks_vmem[0].shape[2]
    offset = 0
    for ref in blocks_vmem:
        count = ref.shape[1]
        for q in range(PIECES):
            held[offset : offset + count, q * piece : (q + 1) * piece] = ref[first_part + q]
        offset += count


def finish(place, half, my_index, leaving, tile_owner, blocks, w_up, w_down, sums, moments):
    arrays = flatten(blocks)
    width, hidden_units = w_up.shape
    tiles = tile_owner.shape[0]
    tile_rows = width // tiles
    total = sum(first.shape[1] for _, first, _ in blocks)
    step = width // PIECES
    each = tiles // PIECES
    count = len(blocks)
    rest = (w_up, w_down, sums[1], moments[2], moments[3], sums[0], moments[0], moments[1])

    def body(place_ref, half_ref, me, leave, owner, *refs):
        block_refs, refs = refs[: len(arrays)], refs[len(arrays) :]
        rest_in, refs = refs[: len(rest)], refs[len(rest) :]
        out_up, out_down, out_near, out_far = refs[:4]
        refs = refs[4:]
        rows_vmem, refs = refs[:count], refs[count:]
        rest_vmem, refs = refs[: len(rest)], refs[len(rest) :]
        up_ref, down_ref, old_down, md, vd, old_up, mu, vu = rest_vmem
        moved_up, moved_down, both, held_x, held_c, held_pre, held_hid = refs[:7]
        sems, up_sems, down_sems, tile_sems = refs[7:]
        starts, waits = pick_copies(place_ref[0], blocks, block_refs, rows_vmem, sems)
        others = [
            pltpu.make_async_copy(source, target, sems.at[count + i])
            for i, (source, target) in enumerate(zip(rest_in, rest_vmem))
        ]
        for start in starts:
            start()
        for copy in others:
            copy.start()
        keep = me[0] != leave[0]
        for copy in waits:
            copy.wait()
        lay_rows(rows_vmem, held_x, 0)
        lay_rows(rows_vmem, held_c, PIECES)
        for copy in others[:2]:
            copy.wait()
        row_terms(up_ref, down_ref, held_x, held_c, held_pre, held_hid, total)
        for copy in others[2:5]:
            copy.wait()

        def leave_steps(j):
            span = pl.ds(pl.multiple_of(j * step, step), step)
            return (
                pltpu.make_async_copy(moved_up.at[span, :], out_up.at[span, :], up_sems.at[j]),
                pltpu.make_async_copy(moved_down.at[:, span], out_down.at[:, span], down_sems.at[j]),
            )

        def tile_copy(t, out):
            span = pl.ds(pl.multiple_of(t * tile_rows, tile_rows), tile_rows)
            return pltpu.make_async_copy(
                both.at[span, :], out.at[owner[t] >> 1], tile_sems.at[t]
            )

        def down_columns(j, carry):
            span = pl.ds(pl.multiple_of(j * step, step), step)
            grad = old_down[:, span] + column_sums(held_hid[...], held_c[:, span])
            step_down = adam_step(grad, md[:, span], vd[:, span])
            both[span, hidden_units:] = step_down.T.astype(jnp.bfloat16)
            moved_down[:, span] = jnp.where(keep, step_down, 0.0).astype(jnp.bfloat16)
            leave_steps(j)[1].start()
            return carry

        def up_columns(j, carry):
            span = pl.ds(pl.multiple_of(j * step, step), step)
            grad = old_up[:, span] + column_sums(held_pre[...], held_x[:, span])
            step_up = adam_step(grad.T, mu[span, :], vu[span, :])
            both[span, :hidden_units] = step_up.astype(jnp.bfloat16)
            moved_up[span, :] = jnp.where(keep, step_up, 0.0).astype(jnp.bfloat16)
            for k in range(each):
                t = j * each + k
                near = (owner[t] & 1) == half_ref[0]
                pl.when(near)(tile_copy(t, out_near).start)
                pl.when(jnp.logical_not(near))(tile_copy(t, out_far).start)
            leave_steps(j)[0].start()
            return carry

        def drain(j, carry):
            for copy in leave_steps(j):
                copy.wait()
            for k in range(each):
                tile_copy(j * each + k, out_near).wait()
            return carry

        lax.fori_loop(0, PIECES, down_columns, 0)
        for copy in others[5:]:
            copy.wait()
        lax.fori_loop(0, PIECES, up_columns, 0)
        lax.fori_loop(0, PIECES, drain, 0)

    tile_shape = jax.ShapeDtypeStruct((tiles // 2, tile_rows, 2 * hidden_units), jnp.bfloat16)
    return pl.pallas_call(
        body,
        out_shape=[
            jax.ShapeDtypeStruct((width, hidden_units), jnp.bfloat16),
            jax.ShapeDtypeStruct((hidden_units, width), jnp.bfloat16),
            tile_shape,
            tile_shape,
        ],
        in_specs=[SMEM] * 5 + [HBM] * (len(arrays) + len(rest)),
        out_specs=[HBM] * 4,
        scratch_shapes=[pltpu.VMEM(first.shape, first.dtype) for _, first, _ in blocks]
        + [pltpu.VMEM(a.shape, a.dtype) for a in rest]
        + [
            pltpu.VMEM((width, hidden_units), jnp.bfloat16),
            pltpu.VMEM((hidden_units, width), jnp.bfloat16),
            pltpu.VMEM((width, 2 * hidden_units), jnp.bfloat16),
            pltpu.VMEM((total, width), jnp.bfloat16),
            pltpu.VMEM((total, width), jnp.bfloat16),
            pltpu.VMEM((total, hidden_units), jnp.bfloat16),
            pltpu.VMEM((total, hidden_units), jnp.bfloat16),
            pltpu.SemaphoreType.DMA((count + len(rest),)),
            pltpu.SemaphoreType.DMA((PIECES,)),
            pltpu.SemaphoreType.DMA((PIECES,)),
            pltpu.SemaphoreType.DMA((tiles,)),
        ],
        compiler_params=pltpu.CompilerParams(vmem_limit_bytes=LIMIT),
        name="finish",
    )(place, half, my_index, leaving, tile_owner, *arrays, *rest)


def on_device(
    tokens, cotangent, gates, routes, w_up, w_down, m_up, v_up, m_down, v_down, leaving, tile_owner
):
    tok_count, width = tokens.shape
    piece = width // PIECES
    core = lax.axis_index("co")
    low = lax.axis_index("zl")
    half = lax.axis_index("zh")
    column = lax.axis_index(("y", "x"))
    place = jnp.where(core == 0, low, 3 - low)
    base = jnp.where(low <= 1, half, 1 - half)
    place_ref = place.reshape(1)

    outgoing = []
    for tag, group in zip(TAGS, SLOT_GROUPS):
        outgoing += prepare(
            base.reshape(1),
            tokens,
            cotangent,
            gates.reshape(1, tok_count),
            routes.reshape(1, tok_count),
            (group,),
        )

    def step(value, places):
        return lax.ppermute(value, ALL, stream_pairs(places))

    def swap(value):
        return lax.ppermute(value, ALL, swap_pairs())

    chunks = []
    previous = None
    for tag, (_, slots), sent in zip(TAGS, SLOT_GROUPS, outgoing):
        rows = sent.shape[0]
        if previous is not None:
            previous, sent = lax.optimization_barrier((previous, sent))
            chunks[-1][0] = previous
        previous = lax.all_to_all(
            sent.reshape(32, rows // 32, piece), ("co", "y", "x"), 0, 0, tiled=True
        ).reshape(rows, piece)
        chunks.append({"tag": tag, "slots": slots, 0: previous})

    def joined(first, second):
        return jnp.where(place == 3, first, second)

    for ch in chunks:
        tag = ch["tag"]
        if tag not in UNSORTED:
            ch[0] = arrange(ch[0], ch["slots"])
        ch[1] = step(ch[0], (0, 1, 2, 3))
        ch["s0"] = swap(ch[0])
        x2 = step(ch["s0"], (2,))
        y2 = step(ch[1], (0, 1, 3))
        ch["s1"] = swap(ch[1])
        x3 = step(ch[1], (2,))
        y3 = step(y2, (0, 1))
        ch[2] = joined(x2, y2)
        ch["s2"] = swap(ch[2])
        x4 = step(y2, (2,))
        y4 = step(y3, (1,))
        ch[3] = joined(x3, y3)
        ch["s3"] = swap(ch[3])
        ch[5] = step(y3, (2,))
        ch[4] = joined(x4, y4)
        ch["s4"] = swap(ch[4])
        ch[6] = step(y4, (2,))
        ch["s5"] = swap(ch[5])
        ch["s6"] = swap(ch[6])

    rules = {
        "o": (lambda at: at <= 1, 0, "s0"),
        "1": (lambda at: at < 3, 1, None),
        "p": (lambda at: at > 0, "s1", None),
        "2": (None, 2, None),
        "q": (None, "s2", None),
        "3": (None, 3, None),
        "r": (None, "s3", None),
        "4": (lambda at: at >= 2, 4, "s4"),
        "5": (lambda at: at == 3, 5, "s5"),
        "6": (lambda at: at == 3, 6, "s6"),
    }

    def blocks_of(words):
        blocks = []
        for word in words.split():
            ch = chunks[TAGS.index(word[0])]
            for letter in word[1:]:
                test, one, two = rules[letter]
                blocks.append((test, ch[one], None if two is None else ch[two]))
        return blocks

    sums = None
    for words in SUMS:
        sums = absorb(place_ref, blocks_of(words), w_up[0], w_down[0], sums)
    my_index = (column * 2 + half).reshape(1)
    leaver = leaving[0]

    update_up, update_down, near, far = finish(
        place_ref,
        half.reshape(1),
        my_index,
        leaving,
        tile_owner,
        blocks_of(LAST),
        w_up[0],
        w_down[0],
        sums,
        (m_up[0], v_up[0], m_down[0], v_down[0]),
    )

    def from_leaver(tiles):
        incoming = lax.all_to_all(tiles, ("y", "x"), 0, 0, tiled=True)
        return lax.dynamic_index_in_dim(incoming, leaver // 2, 0, keepdims=False)

    far, near = lax.optimization_barrier((far, near))
    far = from_leaver(far)
    crossed = lax.ppermute(far, ALL, across_pairs())
    near = from_leaver(near)
    mine = jnp.where(half == leaver % 2, near, crossed)[None]
    units = w_up.shape[2]
    return (update_up[None], update_down[None], mine[..., :units], mine[..., units:])


def solution(mesh):
    wide = Mesh(mesh.devices.reshape(4, 2, 4, 4, 2), ALL)
    dp = ("zl", "co")
    expert = ("y", "x", "zh")
    row = P(dp + expert, None)
    up = P(expert, None, dp)
    down = P(expert, dp, None)
    return jax.shard_map(
        on_device,
        mesh=wide,
        in_specs=(row, row, row, row, up, down, up, up, down, down, P(), P()),
        out_specs=(up, down, up, up),
        check_vma=False,
    )
```
